32 devices in a mesh: face: 4 (over z), tile: 4 (over y, core), lev: 2 (over x).
Axes of the slice: x: 2, y: 2, z: 4, core: 2. Of those that a mesh axis runs over, the one named last changes fastest.
Arguments:
- airflow_components: float32 [2, 36, 32, 512], P(None, 'lev', 'face', 'tile'), may hold values from -4.5 to 4.5, as said below
- heat_state: float32 [36, 32, 512], P('lev', 'face', 'tile'), may hold values from 0.5 to 2
- layer_pressure_depth: float32 [36, 32, 512], P('lev', 'face', 'tile'), may hold values from 0.5 to 2
- constituent_masses: float32 [18, 36, 32, 512], P(None, 'lev', 'face', 'tile'), may hold values from 0.1 to 1
- ground_gravity_potential: float32 [32, 512], P('face', 'tile'), may hold values from -8 to 8
- inverse_mapping_entries: float32 [4, 32, 512], P(None, 'face', 'tile'), may hold values from -4 to 4
- mapping_determinant: float32 [32, 512], P('face', 'tile'), may hold values from 0.5 to 2
- interface_rightangle_rotations: int32 [4, 4, 2], replicated, may hold values from 0 to 3
- interface_flipped_markers: int32 [4, 4, 2], replicated, may hold values from 0 to 1
- corner_block_tally: int32 [4, 4], replicated, may hold values from 3 to 4
Outputs:
- airflow_next: float32 [2, 36, 32, 512], P(None, 'lev', 'face', 'tile')
- heat_state_next: float32 [36, 32, 512], P('lev', 'face', 'tile')
- pressure_depth_next: float32 [36, 32, 512], P('lev', 'face', 'tile')
- constituent_masses_next: float32 [18, 36, 32, 512], P(None, 'lev', 'face', 'tile')
- stepping_bounds: float32 [2], replicated
The draws below stay inside these ranges and needn't reach their ends.
Inputs may be any that keep to these rules, and one draw needn't show every extreme that they name: `airflow_components`: component magnitudes grow across the grid by up to a factor of 9. `interface_rightangle_rotations`: entry [f, t, 0] concerns the boundary between blocks (f, t) and (f+1, t), entry [f, t, 1] the one between (f, t) and (f, t+1). `interface_flipped_markers`: indexed like interface_rightangle_rotations. `corner_block_tally`: entry [f, t] belongs to the corner shared by blocks (f, t), (f+1, t), (f, t+1), (f+1, t+1).
All inputs are finite; a program needn't handle non-finite values.
Results may differ from the reference program's by a relative error of at most 0.00012.
Values sent between devices are 32-bit elements; how exact they have to be, the bound alone decides.
A program may use at most 64 MiB of HBM per device.

```python
import math
import jax
import jax.numpy as jnp
import numpy as np
from jax import lax

QSIZE = 18
MESH_NODE_NORTHS = 32
MESH_NODE_EASTS = 512
LAYER_NUMBER = 36
N_FACE = 4
N_TILE = 4


def draw_airflow_components(key, part):
    row_position = jnp.arange(MESH_NODE_NORTHS, dtype=jnp.float32)[:, None] / MESH_NODE_NORTHS
    column_position = jnp.arange(MESH_NODE_EASTS, dtype=jnp.float32)[None, :] / MESH_NODE_EASTS
    spread_factor = 0.5 * jnp.exp(jnp.log(3.0) * (row_position + column_position))
    standard = jnp.clip(jax.random.normal(key, (2, LAYER_NUMBER, MESH_NODE_NORTHS, MESH_NODE_EASTS), jnp.float32), -3.0, 3.0)
    return (standard * spread_factor / 3.0).astype(jnp.float32)


def touch_ends(drawn, stream_key, smallest, largest):
    longest = drawn.shape.index(max(drawn.shape))
    spots = []
    for shift in (0, 1):
        where = [jax.random.randint(jax.random.fold_in(stream_key, axis), (), 0, length) for axis, length in enumerate(drawn.shape)]
        where[longest] = (where[longest] + shift) % drawn.shape[longest]
        spots.append(tuple(where))
    return drawn.at[spots[0]].set(smallest).at[spots[1]].set(largest)


def steps_of(rng, shape, cuts, low, largest):
    def one(position, blocks):
        heights = jax.random.uniform(jax.random.fold_in(jax.random.fold_in(rng, 6), position), (blocks,), jnp.float32, low / len(cuts), largest / len(cuts))
        return jnp.repeat(jnp.exp(heights), shape[position] // blocks).reshape((-1,) + (1,) * (len(shape) - position - 1))

    level = one(*cuts[0])
    for cut in cuts[1:]:
        level = level * one(*cut)
    return level


def noise(key, extent, spread, bound, split=(), kind=jnp.bfloat16):
    result = spread * jax.random.normal(key, extent, jnp.float32)
    if split:
        result = result * steps_of(key, extent, split, -0.22, 0.18)
    return jnp.clip(result, -bound, bound).astype(kind)


def setup_inputs(seed: int = 0) -> dict:
    splits = jax.random.split(jax.random.key(seed), 11)
    airflow_components = draw_airflow_components(jax.random.fold_in(splits[10], 71), 0)
    heat_state = jnp.clip(jnp.exp(math.log(2.0) - 1.3862944 * jax.random.uniform(splits[1], (LAYER_NUMBER, MESH_NODE_NORTHS, MESH_NODE_EASTS), jnp.float32) ** steps_of(splits[1], (LAYER_NUMBER, MESH_NODE_NORTHS, MESH_NODE_EASTS), ((0, 2), (1, 4), (2, 4)), -0.2, 0.2)), 0.5, 2.0)
    layer_pressure_depth = jnp.clip(jnp.exp(math.log(2.0) - 1.3862944 * jax.random.uniform(splits[2], (LAYER_NUMBER, MESH_NODE_NORTHS, MESH_NODE_EASTS), jnp.float32) ** steps_of(splits[2], (LAYER_NUMBER, MESH_NODE_NORTHS, MESH_NODE_EASTS), ((0, 2), (1, 4), (2, 4)), -0.2, 0.2)), 0.5, 2.0)
    constituent_masses = jnp.clip(jnp.exp(math.log(1.0) - 2.3025851 * jax.random.uniform(splits[3], (QSIZE, LAYER_NUMBER, MESH_NODE_NORTHS, MESH_NODE_EASTS), jnp.float32) ** steps_of(splits[3], (QSIZE, LAYER_NUMBER, MESH_NODE_NORTHS, MESH_NODE_EASTS), ((1, 2), (2, 4), (3, 4)), -0.2, 0.2)), 0.1, 1.0)
    ground_gravity_potential = noise(splits[4], (MESH_NODE_NORTHS, MESH_NODE_EASTS), 2.0, 8.0, ((0, 4), (1, 4)), jnp.float32)
    inverse_mapping_entries = noise(splits[5], (4, MESH_NODE_NORTHS, MESH_NODE_EASTS), 1.0, 4.0, ((1, 4), (2, 4)), jnp.float32)
    mapping_determinant = jnp.clip(jnp.exp(math.log(2.0) - 1.3862944 * jax.random.uniform(splits[6], (MESH_NODE_NORTHS, MESH_NODE_EASTS), jnp.float32) ** steps_of(splits[6], (MESH_NODE_NORTHS, MESH_NODE_EASTS), ((0, 4), (1, 4)), -0.2, 0.2)), 0.5, 2.0)
    interface_rightangle_rotations = touch_ends(jax.random.randint(splits[7], (N_FACE, N_TILE, 2), 0, 4), jax.random.fold_in(splits[7], 1), 0, 3).astype(jnp.int32)
    interface_flipped_markers = touch_ends(jax.random.randint(splits[8], (N_FACE, N_TILE, 2), 0, 2), jax.random.fold_in(splits[8], 1), 0, 1).astype(jnp.int32)
    corner_block_tally = touch_ends(jax.random.randint(splits[9], (N_FACE, N_TILE), 3, 5), jax.random.fold_in(splits[9], 1), 3, 4).astype(jnp.int32)
    return dict(airflow_components=airflow_components, heat_state=heat_state, layer_pressure_depth=layer_pressure_depth, constituent_masses=constituent_masses, ground_gravity_potential=ground_gravity_potential, inverse_mapping_entries=inverse_mapping_entries, mapping_determinant=mapping_determinant, interface_rightangle_rotations=interface_rightangle_rotations, interface_flipped_markers=interface_flipped_markers, corner_block_tally=corner_block_tally)


time_step = 0.05
viscosity = 0.05
highest = lax.Precision.HIGHEST

def gll_tables():
    offset = 1.0 / math.sqrt(5.0)
    gll_nodes = np.array([-1.0, -offset, offset, 1.0])
    weights = np.array([1.0 / 6.0, 5.0 / 6.0, 5.0 / 6.0, 1.0 / 6.0])
    barycentric = np.ones(4)
    for outer_index in range(4):
        for inner_index in range(4):
            if inner_index != outer_index:
                barycentric[outer_index] = barycentric[outer_index] / (gll_nodes[outer_index] - gll_nodes[inner_index])
    derivative = np.zeros((4, 4))
    for outer_index in range(4):
        for inner_index in range(4):
            if inner_index != outer_index:
                derivative[outer_index, inner_index] = barycentric[inner_index] / barycentric[outer_index] / (gll_nodes[outer_index] - gll_nodes[inner_index])
        derivative[outer_index, outer_index] = -np.sum(derivative[outer_index])
    return (derivative, weights)

def advance(east_wind, north_wind, temp_field, thick_field, tracer_field, geo_field, inverse_mapping_entries, mapping_determinant, along_rows, along_columns):

    def gradient(scalar):
        first_part = along_rows(scalar)
        second_part = along_columns(scalar)
        return (inverse_mapping_entries[0] * first_part + inverse_mapping_entries[2] * second_part, inverse_mapping_entries[1] * first_part + inverse_mapping_entries[3] * second_part)

    def divergence(east_part, north_part):
        first_flux = mapping_determinant * (inverse_mapping_entries[0] * east_part + inverse_mapping_entries[1] * north_part)
        second_flux = mapping_determinant * (inverse_mapping_entries[2] * east_part + inverse_mapping_entries[3] * north_part)
        return (along_rows(first_flux) + along_columns(second_flux)) / mapping_determinant
    energy = 0.5 * (east_wind * east_wind + north_wind * north_wind) + geo_field
    energy_x, energy_y = gradient(energy)
    temp_x, temp_y = gradient(temp_field)
    thick_x, thick_y = gradient(thick_field)
    laplace = divergence(thick_x, thick_y)
    new_east = east_wind - time_step * energy_x
    new_north = north_wind - time_step * energy_y
    new_temp = temp_field - time_step * (east_wind * temp_x + north_wind * temp_y)
    new_thick = thick_field - time_step * divergence(thick_field * east_wind, thick_field * north_wind) + time_step * viscosity * laplace
    new_tracer = tracer_field - time_step * divergence(tracer_field * east_wind, tracer_field * north_wind)
    spacing = jnp.sqrt(inverse_mapping_entries[0] * inverse_mapping_entries[0] + inverse_mapping_entries[1] * inverse_mapping_entries[1] + inverse_mapping_entries[2] * inverse_mapping_entries[2] + inverse_mapping_entries[3] * inverse_mapping_entries[3])
    courant = jnp.max(time_step * jnp.sqrt(east_wind * east_wind + north_wind * north_wind) * spacing)
    damping = jnp.max(time_step * viscosity * jnp.abs(laplace))
    fields = jnp.concatenate([new_east[None], new_north[None], new_temp[None], new_thick[None], new_tracer], 0)
    return (fields, courant, damping)

def turn(pieces, code):
    cosine = jnp.where(code == 0, 1.0, jnp.where(code == 2, -1.0, 0.0)).astype(jnp.float32)
    sine = jnp.where(code == 1, 1.0, jnp.where(code == 3, -1.0, 0.0)).astype(jnp.float32)
    first_part = cosine * pieces[0] - sine * pieces[1]
    second_part = sine * pieces[0] + cosine * pieces[1]
    return jnp.concatenate([first_part[None], second_part[None], pieces[2:]], 0)

def flip_edge(strip, flag):
    return jnp.where(flag[..., None] == 1, strip[..., ::-1], strip)

def fix_edge(strip, flag, code):
    return turn(flip_edge(strip, flag), code[..., None])

def assemble(inner, top_rim, bottom_rim, left_rim, right_rim, corner_ll, corner_lh, corner_hl, corner_hh):
    first_row = jnp.concatenate([corner_ll[..., None], top_rim, corner_lh[..., None]], -1)
    last_row = jnp.concatenate([corner_hl[..., None], bottom_rim, corner_hh[..., None]], -1)
    middle = jnp.concatenate([left_rim[..., None], inner, right_rim[..., None]], -1)
    return jnp.concatenate([first_row[..., None, :], middle, last_row[..., None, :]], -2)

def shared_sums(padded):
    row_count = padded.shape[-2] - 2
    column_count = padded.shape[-1] - 2
    row_low = (jnp.arange(row_count) % 4 == 0)[:, None]
    row_high = (jnp.arange(row_count) % 4 == 3)[:, None]
    across = padded[..., 1:-1, :] + jnp.where(row_low, padded[..., :-2, :], 0.0) + jnp.where(row_high, padded[..., 2:, :], 0.0)
    column_low = jnp.arange(column_count) % 4 == 0
    column_high = jnp.arange(column_count) % 4 == 3
    return across[..., 1:-1] + jnp.where(column_low, across[..., :-2], 0.0) + jnp.where(column_high, across[..., 2:], 0.0)

def combine_block(pieces, mass_pieces, rotations, flips, valences):
    inner, top_rim, bottom_rim, left_rim, right_rim, corner_ll, corner_lh, corner_hl, corner_hh = pieces
    mass_inner, mass_top, mass_bottom, mass_left, mass_right, mass_ll, mass_lh, mass_hl, mass_hh = mass_pieces
    top_code, bottom_code, left_code, right_code = rotations
    top_flag, bottom_flag, left_flag, right_flag = flips
    valence_ll, valence_lh, valence_hl, valence_hh = valences
    fixed = assemble(inner, fix_edge(top_rim, top_flag, top_code), fix_edge(bottom_rim, bottom_flag, bottom_code), fix_edge(left_rim, left_flag, left_code), fix_edge(right_rim, right_flag, right_code), jnp.where(valence_ll == 4, turn(corner_ll, (top_code + left_code) % 4), 0.0), jnp.where(valence_lh == 4, turn(corner_lh, (top_code + right_code) % 4), 0.0), jnp.where(valence_hl == 4, turn(corner_hl, (bottom_code + left_code) % 4), 0.0), jnp.where(valence_hh == 4, turn(corner_hh, (bottom_code + right_code) % 4), 0.0))
    mass_fixed = assemble(mass_inner, flip_edge(mass_top, top_flag), flip_edge(mass_bottom, bottom_flag), flip_edge(mass_left, left_flag), flip_edge(mass_right, right_flag), jnp.where(valence_ll == 4, mass_ll, 0.0), jnp.where(valence_lh == 4, mass_lh, 0.0), jnp.where(valence_hl == 4, mass_hl, 0.0), jnp.where(valence_hh == 4, mass_hh, 0.0))
    return shared_sums(fixed) / shared_sums(mass_fixed)

def block_pieces(field, face_count, tile_count):
    field_count = field.shape[0]
    row_count = field.shape[1] // face_count
    column_count = field.shape[2] // tile_count
    blocks = field.reshape(field_count, face_count, row_count, tile_count, column_count).transpose(0, 1, 3, 2, 4)
    top_rim = jnp.roll(blocks[:, :, :, -1, :], 1, axis=1)
    bottom_rim = jnp.roll(blocks[:, :, :, 0, :], -1, axis=1)
    left_rim = jnp.roll(blocks[:, :, :, :, -1], 1, axis=2)
    right_rim = jnp.roll(blocks[:, :, :, :, 0], -1, axis=2)
    corner_ll = jnp.roll(jnp.roll(blocks[:, :, :, -1, -1], 1, axis=1), 1, axis=2)
    corner_lh = jnp.roll(jnp.roll(blocks[:, :, :, -1, 0], 1, axis=1), -1, axis=2)
    corner_hl = jnp.roll(jnp.roll(blocks[:, :, :, 0, -1], -1, axis=1), 1, axis=2)
    corner_hh = jnp.roll(jnp.roll(blocks[:, :, :, 0, 0], -1, axis=1), -1, axis=2)
    return (blocks, top_rim, bottom_rim, left_rim, right_rim, corner_ll, corner_lh, corner_hl, corner_hh)

def reference(airflow_components, heat_state, layer_pressure_depth, constituent_masses, ground_gravity_potential, inverse_mapping_entries, mapping_determinant, interface_rightangle_rotations, interface_flipped_markers, corner_block_tally):
    derivative, weights = gll_tables()
    deriv_table = jnp.asarray(derivative, jnp.float32)

    def along_rows(field):
        field_shape = field.shape
        blocks = field.reshape(field_shape[:-2] + (field_shape[-2] // 4, 4, field_shape[-1]))
        return jnp.einsum('ab,...ebc->...eac', deriv_table, blocks, precision=highest).reshape(field_shape)

    def along_columns(field):
        field_shape = field.shape
        blocks = field.reshape(field_shape[:-1] + (field_shape[-1] // 4, 4))
        return jnp.einsum('ab,...eb->...ea', deriv_table, blocks, precision=highest).reshape(field_shape)
    strip_parts_sequence = heat_state * layer_pressure_depth
    column_total = lax.optimization_barrier(jnp.sum(strip_parts_sequence, axis=0))
    gravity_potential_altitude = ground_gravity_potential + (column_total - jnp.cumsum(strip_parts_sequence, axis=0)) + 0.5 * strip_parts_sequence
    grid_rows = mapping_determinant.shape[0]
    grid_columns = mapping_determinant.shape[1]
    weight_rows = jnp.asarray(np.tile(weights, grid_rows // 4), jnp.float32)
    weight_columns = jnp.asarray(np.tile(weights, grid_columns // 4), jnp.float32)
    mass = mapping_determinant * weight_rows[:, None] * weight_columns[None, :]
    turns_rows = interface_rightangle_rotations[:, :, 0]
    turns_columns = interface_rightangle_rotations[:, :, 1]
    rotations = ((4 - jnp.roll(turns_rows, 1, axis=0)) % 4, turns_rows, (4 - jnp.roll(turns_columns, 1, axis=1)) % 4, turns_columns)
    flips = (jnp.roll(interface_flipped_markers[:, :, 0], 1, axis=0), interface_flipped_markers[:, :, 0], jnp.roll(interface_flipped_markers[:, :, 1], 1, axis=1), interface_flipped_markers[:, :, 1])
    valences = (jnp.roll(jnp.roll(corner_block_tally, 1, axis=0), 1, axis=1), jnp.roll(corner_block_tally, 1, axis=0), jnp.roll(corner_block_tally, 1, axis=1), corner_block_tally)
    mass_pieces = block_pieces(mass[None], N_FACE, N_TILE)

    def lone_layer(level_inputs):
        wind_pair, temp_level, thick_level, tracer_level, geo_level = level_inputs
        fields, courant, damping = advance(wind_pair[0], wind_pair[1], temp_level, thick_level, tracer_level, geo_level, inverse_mapping_entries, mapping_determinant, along_rows, along_columns)
        pieces = block_pieces(fields * mass, N_FACE, N_TILE)
        substep_outcome = combine_block(pieces, mass_pieces, rotations, flips, valences)
        field_count = substep_outcome.shape[0]
        return (substep_outcome.transpose(0, 1, 3, 2, 4).reshape(field_count, grid_rows, grid_columns), courant, damping)
    piled_layers, stepwise_advection_number_layerwise, hyperdiffusion_change_layerwise = lax.map(lone_layer, (jnp.moveaxis(airflow_components, 1, 0), heat_state, layer_pressure_depth, jnp.moveaxis(constituent_masses, 1, 0), gravity_potential_altitude))
    airflow_next = jnp.moveaxis(piled_layers[:, 0:2], 0, 1)
    heat_state_next = piled_layers[:, 2]
    pressure_depth_next = piled_layers[:, 3]
    constituent_masses_next = jnp.moveaxis(piled_layers[:, 4:], 0, 1)
    stepping_bounds = jnp.stack([jnp.max(stepwise_advection_number_layerwise), jnp.max(hyperdiffusion_change_layerwise)])
    return (airflow_next, heat_state_next, pressure_depth_next, constituent_masses_next, stepping_bounds)
```

```python
import functools
import math

import jax
import jax.numpy as jnp
import numpy as np
from jax import lax
from jax.experimental import pallas as pl
from jax.experimental.pallas import tpu as pltpu
from jax.sharding import PartitionSpec as P

time_step = 0.05
viscosity = 0.05
f32 = jnp.float32
bf16 = jnp.bfloat16
MESH = pl.DeviceIdType.MESH
highest = lax.Precision.HIGHEST


def gll_tables():
    offset = 1.0 / math.sqrt(5.0)
    nodes = np.array([-1.0, -offset, offset, 1.0])
    weights = np.array([1.0 / 6.0, 5.0 / 6.0, 5.0 / 6.0, 1.0 / 6.0])
    bary = np.ones(4)
    for i in range(4):
        for j in range(4):
            if j != i:
                bary[i] = bary[i] / (nodes[i] - nodes[j])
    derivative = np.zeros((4, 4))
    for i in range(4):
        for j in range(4):
            if j != i:
                derivative[i, j] = bary[j] / bary[i] / (nodes[i] - nodes[j])
        derivative[i, i] = -np.sum(derivative[i])
    return derivative, weights


def lane_tables(columns):
    derivative, weights = gll_tables()
    d = np.kron(np.eye(columns // 4), derivative)
    s = np.eye(columns)
    for c in range(columns - 1):
        if c % 4 == 3:
            s[c, c + 1] = s[c + 1, c] = 1.0
    w = np.tile(weights, columns // 4)
    t = (-time_step * (d.T * w[None, :]) @ s).astype(np.float32)
    t_hi = jnp.asarray(t).astype(bf16)
    t_lo = (jnp.asarray(t) - t_hi.astype(f32)).astype(bf16)
    sb = jnp.asarray(s, bf16)
    return jnp.concatenate([sb, sb, t_hi, t_hi, t_lo], 0), jnp.asarray(d.T, f32), jnp.asarray(w[None, :], f32)


def split(x):
    hi = x.astype(bf16)
    return hi, (x - hi.astype(f32)).astype(bf16)


def layout(levels, tracers):
    group = 8 // math.gcd(levels, 8)
    chunks, q = [], 0
    while q < tracers:
        n = min(group, tracers - q)
        chunks.append((q * levels, -(-n * levels // 8) * 8, n * levels))
        q += n
    return chunks


def kernel(
    sizes, dims,
    wind_h, temp_h, thick_h, tracer_h, ground_h, maps_h, det_h, ops_h, dct_h, wc_h,
    rot_ref, flip_ref, tally_ref,
    wind_o, temp_o, thick_o, tracer_o, bound_o,
    wind, temp, thick, tracer, geo, ground, maps, det, ops, dct, wc,
    a_ref, b_ref, z_ref, pack, corner, total, peak,
    up_in, down_in, left_in, right_in, corner_in, total_in, peak_in,
    in_sem, up_s, up_r, down_s, down_r, left_s, left_r, right_s, right_r,
    corner_s, corner_r, total_s, total_r, peak_s, peak_r,
):
    nf, nt, nl = sizes
    levels, rows, columns, chunks, pad = dims
    derivative, weights = gll_tables()
    rep = [a - (a // 4) for a in range(rows)]
    distinct = rows - rows // 4 + 1
    face, tile, lev = lax.axis_index("face"), lax.axis_index("tile"), lax.axis_index("lev")
    f_up, f_dn = lax.rem(face + nf - 1, nf), lax.rem(face + 1, nf)
    t_lf, t_rt = lax.rem(tile + nt - 1, nt), lax.rem(tile + 1, nt)

    pieces = [(0, 2 * pad + 8, 1)]
    at = 2 * pad + 8
    for _, count, _ in chunks:
        pieces.append((at, count, 1))
        at += count
    pieces.append((at, 2 * pad, 2))
    first_pack = np.cumsum([0] + [p[2] for p in pieces]).tolist()
    last = len(pieces) - 1

    local = [
        (temp_h, temp.at[: levels * rows]), (thick_h, thick.at[: levels * rows]),
        (wind_h.at[0], wind.at[0, : levels * rows]), (wind_h.at[1], wind.at[1, : levels * rows]),
        (maps_h, maps), (det_h, det), (wc_h, wc), (ground_h, ground), (dct_h, dct), (ops_h, ops),
    ]
    loads = [pltpu.make_async_copy(s, d, in_sem.at[i]) for i, (s, d) in enumerate(local)]
    n0 = len(local)
    for k, (start, _, valid) in enumerate(chunks):
        span = pl.ds(start * rows, valid * rows)
        loads.append(pltpu.make_async_copy(tracer_h.at[span], tracer.at[span], in_sem.at[n0 + k]))
    for load in loads:
        load.start()

    peers = [(lax.rem(face + o, nf), tile, lev) for o in range(1, nf)]
    peers += [(face, lax.rem(tile + o, nt), lev) for o in range(1, nt)]
    peers += [(face, tile, lax.rem(lev + o, nl)) for o in range(1, nl)]
    diagonals = [(f_dn, t_rt, lev), (f_dn, t_lf, lev), (f_up, t_rt, lev), (f_up, t_lf, lev)]
    barrier = pltpu.get_barrier_semaphore()
    for peer in peers + diagonals:
        pl.semaphore_signal(barrier, inc=1, device_id=peer, device_id_type=MESH)

    extra = (pad - levels) * rows
    if extra:
        zero = jnp.zeros((extra, columns), f32)
        temp[levels * rows :, :] = zero
        thick[levels * rows :, :] = zero
        geo[levels * rows :, :] = zero
        wind[0, levels * rows :, :] = zero
        wind[1, levels * rows :, :] = zero
    end = chunks[-1][0] + chunks[-1][2]
    more = chunks[-1][1] - chunks[-1][2]
    if more:
        tracer[end * rows :, :] = jnp.zeros((more * rows, columns), f32)

    sent = []

    def send(src, dst, s, r, to):
        copy = pltpu.make_async_remote_copy(
            src_ref=src, dst_ref=dst, send_sem=s, recv_sem=r, device_id=to, device_id_type=MESH
        )
        copy.start()
        sent.append(copy)
        return copy

    loads[0].wait()
    loads[1].wait()
    acc = jnp.zeros((rows, columns), f32)
    for k in reversed(range(levels)):
        term = temp[k * rows : (k + 1) * rows, :] * thick[k * rows : (k + 1) * rows, :]
        geo[k * rows : (k + 1) * rows, :] = acc + 0.5 * term
        acc = acc + term
    total[...] = acc
    pl.semaphore_wait(barrier, len(peers) + len(diagonals))
    totals = [
        send(total, total_in.at[o - 1], total_s.at[o - 1], total_r.at[o - 1],
             (face, tile, lax.rem(lev + o, nl)))
        for o in range(1, nl)
    ]

    for load in loads[2:n0]:
        load.wait()
    w_col = wc[...]
    table = ops[...]
    narrow = ops[: 2 * columns, :]
    wr = [float(weights[a % 4]) for a in range(rows)]
    m = [[maps[e * rows + a : e * rows + a + 1, :] for a in range(rows)] for e in range(4)]
    jac = [det[a : a + 1, :] for a in range(rows)]
    mass = [jac[a] * (wr[a] * w_col) for a in range(rows)]
    step_d = [[float(time_step * wr[a] * derivative[a % 4, b]) for b in range(4)] for a in range(rows)]
    dd = [[float(derivative[i, j]) for j in range(4)] for i in range(4)]

    def level_rows(ref, a):
        return ref[pl.ds(a, pad, stride=rows), :]

    def along_rows(values, a, coef):
        base = a - a % 4
        out = coef[0] * values[base]
        for b in range(1, 4):
            out = out + coef[b] * values[base + b]
        return out

    def merged(values):
        out = [None] * distinct
        for a in range(rows):
            r = rep[a]
            out[r] = values[a] if out[r] is None else out[r] + values[a]
        return out

    def lanes_plain(x):
        hi, lo = split(x)
        return jnp.dot(jnp.concatenate([hi, lo], 1), narrow, preferred_element_type=f32)

    def lanes_both(p, g):
        ph, plo = split(p)
        gh, glo = split(g)
        return jnp.dot(
            jnp.concatenate([ph, plo, gh, glo, gh], 1), table, preferred_element_type=f32
        )

    def by_column(values):
        stacked = jnp.concatenate(values, 0)
        out = jnp.dot(stacked, dct[...], precision=highest, preferred_element_type=f32)
        n = values[0].shape[0]
        return [out[i * n : (i + 1) * n] for i in range(len(values))]

    lane = lax.broadcasted_iota(jnp.int32, (8, columns), 1)
    unit = 2 * distinct
    within = lax.rem(lane, unit)

    def put(piece, offset, r, z):
        z_ref[r, piece + offset : piece + offset + z.shape[0], :] = z

    def pack_of(start, groups):
        out = jnp.zeros((8, columns), f32)
        for i in range(groups):
            for r in range(distinct):
                spot = unit * i + 2 * r
                value = pltpu.roll(z_ref[r, start + 8 * i : start + 8 * i + 8, :], spot + 1, 1)
                out = jnp.where((lane == spot) | (lane == spot + 1), value, out)
        return out

    def ship(j):
        start, count, packs = pieces[j]
        span = pl.ds(start, count)
        send(z_ref.at[distinct - 1, span], up_in.at[span], up_s.at[j], up_r.at[j], (f_dn, tile, lev))
        send(z_ref.at[0, span], down_in.at[span], down_s.at[j], down_r.at[j], (f_up, tile, lev))
        each = count // packs
        made = []
        for p in range(packs):
            made.append(pack_of(start + p * each, each // 8))
            pack[first_pack[j] + p] = made[-1]
        span = pl.ds(first_pack[j], packs)
        send(pack.at[span], left_in.at[span], left_s.at[j], left_r.at[j], (face, t_rt, lev))
        send(pack.at[span], right_in.at[span], right_s.at[j], right_r.at[j], (face, t_lf, lev))
        return made

    source = [unit - 2, unit - 1, 0, 1]

    def ship_corners(which, made):
        for d in range(4):
            out = jnp.zeros((8, columns), f32)
            for p, value in enumerate(made):
                out = jnp.where(within == p, pltpu.roll(value, (p - source[d]) % columns, 1), out)
            corner[which, d] = out
            send(corner.at[which, d], corner_in.at[which, d], corner_s.at[which, d],
                 corner_r.at[which, d], diagonals[d])

    east = [level_rows(wind.at[0], a) for a in range(rows)]
    north = [level_rows(wind.at[1], a) for a in range(rows)]
    speed = None
    whole = max(c[1] for c in chunks)
    for a in range(rows):
        aa = jac[a] * (m[0][a] * east[a] + m[1][a] * north[a])
        bb = jac[a] * (m[2][a] * east[a] + m[3][a] * north[a])
        aw, bw = (aa * w_col)[:levels], (bb * wr[a])[:levels]
        for k in range(-(-whole // levels)):
            n = min(levels, whole - k * levels)
            a_ref[a, k * levels : k * levels + n, :] = aw[:n]
            b_ref[a, k * levels : k * levels + n, :] = bw[:n]
        spacing = jnp.sqrt(
            m[0][a] * m[0][a] + m[1][a] * m[1][a] + m[2][a] * m[2][a] + m[3][a] * m[3][a]
        )
        here = jnp.max(east[a] * east[a] + north[a] * north[a], axis=0, keepdims=True)
        here = jnp.sqrt(here) * spacing
        speed = here if speed is None else jnp.maximum(speed, here)

    depth = [level_rows(thick, a) for a in range(rows)]
    depth_c = by_column(depth)
    flux_a, flux_b = [], []
    for a in range(rows):
        dr, dc = along_rows(depth, a, dd[a % 4]), depth_c[a]
        gx, gy = m[0][a] * dr + m[2][a] * dc, m[1][a] * dr + m[3][a] * dc
        flux_a.append(jac[a] * (m[0][a] * gx + m[1][a] * gy))
        flux_b.append(jac[a] * (m[2][a] * gx + m[3][a] * gy))
    flux_c = by_column(flux_b)
    damp = None
    for a in range(rows):
        lap = jnp.abs(along_rows(flux_a, a, dd[a % 4]) + flux_c[a])
        here = jnp.max(lap, axis=0, keepdims=True) / jac[a]
        damp = here if damp is None else jnp.maximum(damp, here)
    peak[0] = jnp.concatenate(
        [time_step * speed, (time_step * viscosity) * damp, jnp.zeros((6, columns), f32)], 0
    )
    peak_face = [
        send(peak.at[0], peak_in.at[o - 1], peak_s.at[o - 1], peak_r.at[o - 1],
             (lax.rem(face + o, nf), tile, lev))
        for o in range(1, nf)
    ]
    warm = [level_rows(temp, a) for a in range(rows)]
    warm_c = by_column(warm)
    value = []
    for a in range(rows):
        dr, dc = along_rows(warm, a, dd[a % 4]), warm_c[a]
        gx, gy = m[0][a] * dr + m[2][a] * dc, m[1][a] * dr + m[3][a] * dc
        value.append(mass[a] * (warm[a] - time_step * (east[a] * gx + north[a] * gy)))
    for r, x in enumerate(merged(value)):
        put(pieces[0][0], 0, r, lanes_plain(x))
    for r, x in enumerate(merged(mass)):
        put(pieces[0][0], pad, r, lanes_plain(jnp.broadcast_to(x, (8, columns))))
    first, second, keep = [], [], []
    for a in range(rows):
        aa = jac[a] * (m[0][a] * east[a] + m[1][a] * north[a])
        bb = jac[a] * (m[2][a] * east[a] + m[3][a] * north[a])
        first.append(w_col * (depth[a] * aa - viscosity * flux_a[a]))
        second.append(wr[a] * (depth[a] * bb - viscosity * flux_b[a]))
    for a in range(rows):
        keep.append(mass[a] * depth[a] - along_rows(first, a, step_d[a]))
    for r, (x, y) in enumerate(zip(merged(keep), merged(second))):
        put(pieces[0][0], pad + 8, r, lanes_both(x, y))
    made = ship(0)

    for k, (start, count, _) in enumerate(chunks):
        loads[n0 + k].wait()
        q = [tracer[pl.ds(start * rows + a, count, stride=rows), :] for a in range(rows)]
        first = [q[a] * a_ref[a, :count, :] for a in range(rows)]
        keep = [mass[a] * q[a] - along_rows(first, a, step_d[a]) for a in range(rows)]
        second = [q[a] * b_ref[a, :count, :] for a in range(rows)]
        for r, (x, y) in enumerate(zip(merged(keep), merged(second))):
            put(pieces[k + 1][0], 0, r, lanes_both(x, y))
        made += ship(k + 1)
    ship_corners(0, made)

    best = peak[0]
    for o, copy in enumerate(peak_face):
        copy.wait_recv()
        best = jnp.maximum(best, peak_in[o])
    peak[1] = best
    base = nf - 1
    peak_tile = [
        send(peak.at[1], peak_in.at[base + o - 1], peak_s.at[base + o - 1], peak_r.at[base + o - 1],
             (face, lax.rem(tile + o, nt), lev))
        for o in range(1, nt)
    ]

    above = ground[...]
    for o, copy in enumerate(totals):
        copy.wait_recv()
        origin = lax.rem(lev + nl - (o + 1), nl)
        use = jnp.where(origin > lev, 1.0, 0.0).astype(f32)
        above = above + use * total_in[o]
    energy = []
    for a in range(rows):
        u, v = level_rows(wind.at[0], a), level_rows(wind.at[1], a)
        energy.append(0.5 * (u * u + v * v) + level_rows(geo, a) + above[a : a + 1, :])
    energy_c = by_column(energy)
    value_u, value_v = [], []
    for a in range(rows):
        u, v = level_rows(wind.at[0], a), level_rows(wind.at[1], a)
        dr, dc = along_rows(energy, a, dd[a % 4]), energy_c[a]
        value_u.append(mass[a] * (u - time_step * (m[0][a] * dr + m[2][a] * dc)))
        value_v.append(mass[a] * (v - time_step * (m[1][a] * dr + m[3][a] * dc)))
    for r, (x, y) in enumerate(zip(merged(value_u), merged(value_v))):
        put(pieces[last][0], 0, r, lanes_plain(x))
        put(pieces[last][0], pad, r, lanes_plain(y))
    ship_corners(1, ship(last))

    best = peak[1]
    for o, copy in enumerate(peak_tile):
        copy.wait_recv()
        best = jnp.maximum(best, peak_in[base + o])
    peak[2] = best
    base = nf + nt - 2
    peak_lev = [
        send(peak.at[2], peak_in.at[base + o - 1], peak_s.at[base + o - 1], peak_r.at[base + o - 1],
             (face, tile, lax.rem(lev + o, nl)))
        for o in range(1, nl)
    ]

    def seam(ref, f, t, k):
        return ref[(f * nt + t) * 2 + k]

    codes = [
        lax.rem(4 - seam(rot_ref, f_up, tile, 0), 4), seam(rot_ref, face, tile, 0),
        lax.rem(4 - seam(rot_ref, face, t_lf, 1), 4), seam(rot_ref, face, tile, 1),
    ]
    flips = [
        seam(flip_ref, f_up, tile, 0), seam(flip_ref, face, tile, 0),
        seam(flip_ref, face, t_lf, 1), seam(flip_ref, face, tile, 1),
    ]
    tallies = [
        tally_ref[f_up * nt + t_lf], tally_ref[f_up * nt + tile],
        tally_ref[face * nt + t_lf], tally_ref[face * nt + tile],
    ]

    def cosine(code):
        return jnp.where(code == 0, 1.0, jnp.where(code == 2, -1.0, 0.0)).astype(f32)

    def sine(code):
        return jnp.where(code == 1, 1.0, jnp.where(code == 3, -1.0, 0.0)).astype(f32)

    def filled(x):
        return jnp.full((8, columns), x)

    odd = lax.rem(lane, 2) == 1
    mirror = lane - within + (unit - 2) - 2 * (within // 2) + lax.rem(within, 2)
    mirror = jnp.clip(mirror, 0, columns - 1)
    side_flip = jnp.where(odd, filled(flips[2]), filled(flips[3])) == 1
    side_cos = jnp.where(odd, filled(cosine(codes[2])), filled(cosine(codes[3])))
    side_sin = jnp.where(odd, filled(sine(codes[2])), filled(sine(codes[3])))
    corner_code = [
        lax.rem(codes[0] + codes[2], 4), lax.rem(codes[0] + codes[3], 4),
        lax.rem(codes[1] + codes[2], 4), lax.rem(codes[1] + codes[3], 4),
    ]
    target = [1, 0, unit - 1, unit - 2]
    alive = [filled(tallies[d]) == 4 for d in range(4)]

    def sides(index):
        a, b = left_in[index], right_in[index]
        x = jnp.where(odd, pltpu.roll(a, 1, 1), pltpu.roll(b, columns - 1, 1))
        return jnp.where(side_flip, jnp.take_along_axis(x, mirror, axis=1), x)

    def corner_values(which, d, p):
        x = pltpu.roll(corner_in[which, d], (target[d] - p) % columns, 1)
        return jnp.where(alive[d] & (within == target[d]), x, 0.0)

    edge = (lane[:1] == 0) | (lane[:1] == columns - 1)

    def to_edges(x, i, r):
        y = pltpu.roll(x, (columns - (unit * i + 2 * r + 1)) % columns, 1)
        return jnp.where(edge, y, 0.0)

    rev = (columns - 1) - lax.broadcasted_iota(jnp.int32, (8, columns), 1)
    row_flip = [filled(flips[0]) == 1, filled(flips[1]) == 1]

    def row_rim(ref, which, start, groups):
        out = []
        for i in range(groups):
            x = ref[start + 8 * i : start + 8 * i + 8, :]
            out.append(jnp.where(row_flip[which], jnp.take_along_axis(x, rev, axis=1), x))
        return out

    def arrived(j, corners):
        start, count, packs = pieces[j]
        span, pspan = pl.ds(start, count), pl.ds(first_pack[j], packs)

        def wait(src, dst, s, r, to):
            pltpu.make_async_remote_copy(
                src_ref=src, dst_ref=dst, send_sem=s, recv_sem=r, device_id=to, device_id_type=MESH
            ).wait_recv()

        wait(z_ref.at[distinct - 1, span], up_in.at[span], up_s.at[j], up_r.at[j], (f_dn, tile, lev))
        wait(z_ref.at[0, span], down_in.at[span], down_s.at[j], down_r.at[j], (f_up, tile, lev))
        wait(pack.at[pspan], left_in.at[pspan], left_s.at[j], left_r.at[j], (face, t_rt, lev))
        wait(pack.at[pspan], right_in.at[pspan], right_s.at[j], right_r.at[j], (face, t_lf, lev))
        if corners is not None:
            for d in range(4):
                wait(corner.at[corners, d], corner_in.at[corners, d], corner_s.at[corners, d],
                     corner_r.at[corners, d], diagonals[d])

    def finished(start, i, r, side, i_side, top, bottom):
        x = z_ref[r, start + 8 * i : start + 8 * i + 8, :] + to_edges(side, i_side, r)
        if r == 0:
            x = x + top
        if r == distinct - 1:
            x = x + bottom
        return x

    def store(ref, begin, i, valid, r, x):
        n = min(8, valid - 8 * i)
        if n <= 0:
            return
        for a in range(rows):
            if rep[a] == r:
                ref[pl.ds((begin + 8 * i) * rows + a, n, stride=rows), :] = (x * inverse[a])[:n]

    arrived(0, 0)
    x = sides(first_pack[0])
    for d in range(4):
        x = x + corner_values(0, d, 0)
    groups = pad // 8
    top, bottom = row_rim(up_in, 0, 0, 2 * groups + 1), row_rim(down_in, 1, 0, 2 * groups + 1)
    inverse = [None] * rows
    for r in range(distinct):
        whole_mass = 1.0 / finished(0, groups, r, x, groups, top[groups], bottom[groups])
        for a in range(rows):
            if rep[a] == r:
                inverse[a] = whole_mass
    for i in range(groups):
        for r in range(distinct):
            store(temp_o, 0, i, levels, r, finished(0, i, r, x, i, top[i], bottom[i]))
            j = groups + 1 + i
            store(thick_o, 0, i, levels, r, finished(0, j, r, x, j, top[j], bottom[j]))

    for k, (start, count, valid) in enumerate(chunks):
        j = k + 1
        arrived(j, None)
        x = sides(first_pack[j])
        for d in range(4):
            x = x + corner_values(0, d, j)
        top = row_rim(up_in, 0, pieces[j][0], count // 8)
        bottom = row_rim(down_in, 1, pieces[j][0], count // 8)
        for i in range(count // 8):
            for r in range(distinct):
                store(tracer_o, start, i, valid, r,
                      finished(pieces[j][0], i, r, x, i, top[i], bottom[i]))

    arrived(last, 1)
    p = first_pack[last]
    xu, xv = sides(p), sides(p + 1)
    xu, xv = side_cos * xu - side_sin * xv, side_sin * xu + side_cos * xv
    for d in range(4):
        cu, cv = corner_values(1, d, 0), corner_values(1, d, 1)
        c, s = cosine(corner_code[d]), sine(corner_code[d])
        xu, xv = xu + (c * cu - s * cv), xv + (s * cu + c * cv)
    begin = pieces[last][0]
    rims = []
    for which, ref in ((0, up_in), (1, down_in)):
        both = row_rim(ref, which, begin, 2 * groups)
        c, s = cosine(codes[which]), sine(codes[which])
        ru = [c * both[i] - s * both[groups + i] for i in range(groups)]
        rv = [s * both[i] + c * both[groups + i] for i in range(groups)]
        rims.append((ru, rv))
    for i in range(groups):
        for r in range(distinct):
            store(wind_o.at[0], 0, i, levels, r,
                  finished(begin, i, r, xu, i, rims[0][0][i], rims[1][0][i]))
            store(wind_o.at[1], 0, i, levels, r,
                  finished(begin + pad, i, r, xv, i, rims[0][1][i], rims[1][1][i]))

    best = peak[2]
    for o, copy in enumerate(peak_lev):
        copy.wait_recv()
        best = jnp.maximum(best, peak_in[base + o])
    bound_o[...] = jnp.broadcast_to(jnp.max(best, axis=1, keepdims=True), (8, columns))
    for copy in sent:
        copy.wait_send()


def on_device(
    sizes, wind, temp, thick, tracers, ground, maps, det, rot, flip, tally
):
    nf, nt, nl = sizes
    levels, rows, columns = temp.shape
    if rows != 8 or columns != 128:
        raise ValueError("block shape")
    count = tracers.shape[0]
    chunks = layout(levels, count)
    pad = -(-levels // 8) * 8
    table, dct, w_col = lane_tables(columns)
    distinct = rows - rows // 4 + 1
    total_rows = 4 * pad + 8 + sum(c[1] for c in chunks)
    pieces = len(chunks) + 2
    packs = len(chunks) + 3
    whole = max(c[1] for c in chunks)
    n = levels * rows
    dma = pltpu.SemaphoreType.DMA
    peers = nf + nt + nl - 3
    hbm = pl.BlockSpec(memory_space=pl.ANY)
    smem = pl.BlockSpec(memory_space=pltpu.SMEM)
    vmem = pl.BlockSpec(memory_space=pltpu.VMEM)
    last = chunks[-1]
    outs = pl.pallas_call(
        functools.partial(kernel, sizes, (levels, rows, columns, chunks, pad)),
        out_shape=(
            jax.ShapeDtypeStruct((2, n, columns), f32),
            jax.ShapeDtypeStruct((n, columns), f32),
            jax.ShapeDtypeStruct((n, columns), f32),
            jax.ShapeDtypeStruct((count * n, columns), f32),
            jax.ShapeDtypeStruct((8, columns), f32),
        ),
        in_specs=[hbm] * 10 + [smem] * 3,
        out_specs=(vmem,) * 5,
        scratch_shapes=[
            pltpu.VMEM((2, pad * rows, columns), f32),
            pltpu.VMEM((pad * rows, columns), f32),
            pltpu.VMEM((pad * rows, columns), f32),
            pltpu.VMEM(((last[0] + last[1]) * rows, columns), f32),
            pltpu.VMEM((pad * rows, columns), f32),
            pltpu.VMEM((rows, columns), f32),
            pltpu.VMEM((4 * rows, columns), f32),
            pltpu.VMEM((rows, columns), f32),
            pltpu.VMEM(table.shape, bf16),
            pltpu.VMEM(dct.shape, f32),
            pltpu.VMEM((1, columns), f32),
            pltpu.VMEM((rows, whole, columns), f32),
            pltpu.VMEM((rows, whole, columns), f32),
            pltpu.VMEM((distinct, total_rows, columns), f32),
            pltpu.VMEM((packs, 8, columns), f32),
            pltpu.VMEM((2, 4, 8, columns), f32),
            pltpu.VMEM((rows, columns), f32),
            pltpu.VMEM((3, 8, columns), f32),
            pltpu.VMEM((total_rows, columns), f32),
            pltpu.VMEM((total_rows, columns), f32),
            pltpu.VMEM((packs, 8, columns), f32),
            pltpu.VMEM((packs, 8, columns), f32),
            pltpu.VMEM((2, 4, 8, columns), f32),
            pltpu.VMEM((nl - 1, rows, columns), f32),
            pltpu.VMEM((peers, 8, columns), f32),
            dma((10 + len(chunks),)),
        ]
        + [dma((pieces,))] * 8
        + [dma((2, 4))] * 2
        + [dma((nl - 1,))] * 2
        + [dma((peers,))] * 2,
        compiler_params=pltpu.CompilerParams(collective_id=0, has_side_effects=True),
    )(
        wind.reshape(2, n, columns), temp.reshape(n, columns), thick.reshape(n, columns),
        tracers.reshape(count * n, columns), ground, maps.reshape(4 * rows, columns), det,
        table, dct, w_col, rot.reshape(-1), flip.reshape(-1), tally.reshape(-1),
    )
    return (
        outs[0].reshape(wind.shape), outs[1].reshape(temp.shape), outs[2].reshape(thick.shape),
        outs[3].reshape(tracers.shape), outs[4][:2, 0],
    )


def solution(mesh):
    sizes = tuple(mesh.shape[name] for name in ("face", "tile", "lev"))
    level = P("lev", "face", "tile")
    stacked = P(None, "lev", "face", "tile")
    return jax.shard_map(
        functools.partial(on_device, sizes),
        mesh=mesh,
        in_specs=(stacked, level, level, stacked, P("face", "tile"), P(None, "face", "tile"),
                  P("face", "tile"), P(), P(), P()),
        out_specs=(stacked, level, level, stacked, P()),
        check_vma=False,
    )
```

```python
import functools
import math

import jax
import jax.numpy as jnp
import numpy as np
from jax import lax
from jax.experimental import pallas as pl
from jax.experimental.pallas import tpu as pltpu
from jax.sharding import PartitionSpec as P

time_step = 0.05
viscosity = 0.05
f32 = jnp.float32
bf16 = jnp.bfloat16
MESH = pl.DeviceIdType.MESH
highest = lax.Precision.HIGHEST


def gll_tables():
    offset = 1.0 / math.sqrt(5.0)
    nodes = np.array([-1.0, -offset, offset, 1.0])
    weights = np.array([1.0 / 6.0, 5.0 / 6.0, 5.0 / 6.0, 1.0 / 6.0])
    bary = np.ones(4)
    for i in range(4):
        for j in range(4):
            if j != i:
                bary[i] = bary[i] / (nodes[i] - nodes[j])
    derivative = np.zeros((4, 4))
    for i in range(4):
        for j in range(4):
            if j != i:
                derivative[i, j] = bary[j] / bary[i] / (nodes[i] - nodes[j])
        derivative[i, i] = -np.sum(derivative[i])
    return derivative, weights


def lane_tables(columns):
    derivative, weights = gll_tables()
    d = np.kron(np.eye(columns // 4), derivative)
    s = np.eye(columns)
    for c in range(columns - 1):
        if c % 4 == 3:
            s[c, c + 1] = s[c + 1, c] = 1.0
    w = np.tile(weights, columns // 4)
    t = (-time_step * (d.T * w[None, :]) @ s).astype(np.float32)
    t_hi = jnp.asarray(t).astype(bf16)
    t_lo = (jnp.asarray(t) - t_hi.astype(f32)).astype(bf16)
    sb = jnp.asarray(s, bf16)
    return jnp.concatenate([sb, sb, t_hi, t_hi, t_lo], 0), jnp.asarray(d.T, f32), jnp.asarray(w[None, :], f32)


def split(x):
    hi = x.astype(bf16)
    return hi, (x - hi.astype(f32)).astype(bf16)


def layout(levels, tracers):
    group = 8 // math.gcd(levels, 8)
    chunks, q = [], 0
    while q < tracers:
        n = min(group, tracers - q)
        chunks.append((q * levels, -(-n * levels // 8) * 8, n * levels))
        q += n
    return chunks


def kernel(
    sizes, dims,
    wind_h, temp_h, thick_h, tracer_h, ground_h, maps_h, det_h, ops_h, dct_h, wc_h,
    rot_ref, flip_ref, tally_ref,
    wind_o, temp_o, thick_o, tracer_o, bound_o,
    wind, temp, thick, tracer, geo, ground, maps, det, ops, dct, wc,
    a_ref, b_ref, z_ref, pack, corner, total, peak,
    up_in, down_in, left_in, right_in, corner_in, total_in, peak_in,
    in_sem, up_s, up_r, down_s, down_r, left_s, left_r, right_s, right_r,
    corner_s, corner_r, total_s, total_r, peak_s, peak_r,
):
    nf, nt, nl = sizes
    levels, rows, columns, chunks, pad = dims
    derivative, weights = gll_tables()
    rep = [a - (a // 4) for a in range(rows)]
    distinct = rows - rows // 4 + 1
    face, tile, lev = lax.axis_index("face"), lax.axis_index("tile"), lax.axis_index("lev")
    f_up, f_dn = lax.rem(face + nf - 1, nf), lax.rem(face + 1, nf)
    t_lf, t_rt = lax.rem(tile + nt - 1, nt), lax.rem(tile + 1, nt)

    pieces = [(0, 2 * pad + 8, 1)]
    at = 2 * pad + 8
    for _, count, _ in chunks:
        pieces.append((at, count, 1))
        at += count
    pieces.append((at, 2 * pad, 2))
    first_pack = np.cumsum([0] + [p[2] for p in pieces]).tolist()
    last = len(pieces) - 1

    local = [
        (temp_h, temp.at[: levels * rows]), (thick_h, thick.at[: levels * rows]),
        (wind_h.at[0], wind.at[0, : levels * rows]), (wind_h.at[1], wind.at[1, : levels * rows]),
        (maps_h, maps), (det_h, det), (wc_h, wc), (ground_h, ground), (dct_h, dct), (ops_h, ops),
    ]
    loads = [pltpu.make_async_copy(s, d, in_sem.at[i]) for i, (s, d) in enumerate(local)]
    n0 = len(local)
    for k, (start, _, valid) in enumerate(chunks):
        span = pl.ds(start * rows, valid * rows)
        loads.append(pltpu.make_async_copy(tracer_h.at[span], tracer.at[span], in_sem.at[n0 + k]))
    for load in loads:
        load.start()

    peers = [(lax.rem(face + o, nf), tile, lev) for o in range(1, nf)]
    peers += [(face, lax.rem(tile + o, nt), lev) for o in range(1, nt)]
    peers += [(face, tile, lax.rem(lev + o, nl)) for o in range(1, nl)]
    diagonals = [(f_dn, t_rt, lev), (f_dn, t_lf, lev), (f_up, t_rt, lev), (f_up, t_lf, lev)]
    barrier = pltpu.get_barrier_semaphore()
    for peer in peers + diagonals:
        pl.semaphore_signal(barrier, inc=1, device_id=peer, device_id_type=MESH)

    extra = (pad - levels) * rows
    if extra:
        zero = jnp.zeros((extra, columns), f32)
        temp[levels * rows :, :] = zero
        thick[levels * rows :, :] = zero
        geo[levels * rows :, :] = zero
        wind[0, levels * rows :, :] = zero
        wind[1, levels * rows :, :] = zero
    end = chunks[-1][0] + chunks[-1][2]
    more = chunks[-1][1] - chunks[-1][2]
    if more:
        tracer[end * rows :, :] = jnp.zeros((more * rows, columns), f32)

    sent = []

    def send(src, dst, s, r, to):
        copy = pltpu.make_async_remote_copy(
            src_ref=src, dst_ref=dst, send_sem=s, recv_sem=r, device_id=to, device_id_type=MESH
        )
        copy.start()
        sent.append(copy)
        return copy

    loads[0].wait()
    loads[1].wait()
    acc = jnp.zeros((rows, columns), f32)
    for k in reversed(range(levels)):
        term = temp[k * rows : (k + 1) * rows, :] * thick[k * rows : (k + 1) * rows, :]
        geo[k * rows : (k + 1) * rows, :] = acc + 0.5 * term
        acc = acc + term
    total[...] = acc
    pl.semaphore_wait(barrier, len(peers) + len(diagonals))
    totals = [
        send(total, total_in.at[o - 1], total_s.at[o - 1], total_r.at[o - 1],
             (face, tile, lax.rem(lev + o, nl)))
        for o in range(1, nl)
    ]

    for load in loads[2:n0]:
        load.wait()
    w_col = wc[...]
    table = ops[...]
    narrow = ops[: 2 * columns, :]
    wr = [float(weights[a % 4]) for a in range(rows)]
    m = [[maps[e * rows + a : e * rows + a + 1, :] for a in range(rows)] for e in range(4)]
    jac = [det[a : a + 1, :] for a in range(rows)]
    mass = [jac[a] * (wr[a] * w_col) for a in range(rows)]
    step_d = [[float(time_step * wr[a] * derivative[a % 4, b]) for b in range(4)] for a in range(rows)]
    dd = [[float(derivative[i, j]) for j in range(4)] for i in range(4)]

    def level_rows(ref, a):
        return ref[pl.ds(a, pad, stride=rows), :]

    def along_rows(values, a, coef):
        base = a - a % 4
        out = coef[0] * values[base]
        for b in range(1, 4):
            out = out + coef[b] * values[base + b]
        return out

    def merged(values):
        out = [None] * distinct
        for a in range(rows):
            r = rep[a]
            out[r] = values[a] if out[r] is None else out[r] + values[a]
        return out

    def lanes_plain(x):
        hi, lo = split(x)
        return jnp.dot(jnp.concatenate([hi, lo], 1), narrow, preferred_element_type=f32)

    def lanes_both(p, g):
        ph, plo = split(p)
        gh, glo = split(g)
        return jnp.dot(
            jnp.concatenate([ph, plo, gh, glo, gh], 1), table, preferred_element_type=f32
        )

    def by_column(values):
        stacked = jnp.concatenate(values, 0)
        out = jnp.dot(stacked, dct[...], precision=highest, preferred_element_type=f32)
        n = values[0].shape[0]
        return [out[i * n : (i + 1) * n] for i in range(len(values))]

    lane = lax.broadcasted_iota(jnp.int32, (8, columns), 1)
    unit = 2 * distinct
    within = lax.rem(lane, unit)

    def put(piece, offset, r, z):
        z_ref[r, piece + offset : piece + offset + z.shape[0], :] = z

    def pack_of(start, groups):
        out = jnp.zeros((8, columns), f32)
        for i in range(groups):
            for r in range(distinct):
                spot = unit * i + 2 * r
                value = pltpu.roll(z_ref[r, start + 8 * i : start + 8 * i + 8, :], spot + 1, 1)
                out = jnp.where((lane == spot) | (lane == spot + 1), value, out)
        return out

    def ship(j):
        start, count, packs = pieces[j]
        span = pl.ds(start, count)
        send(z_ref.at[distinct - 1, span], up_in.at[span], up_s.at[j], up_r.at[j], (f_dn, tile, lev))
        send(z_ref.at[0, span], down_in.at[span], down_s.at[j], down_r.at[j], (f_up, tile, lev))
        each = count // packs
        made = []
        for p in range(packs):
            made.append(pack_of(start + p * each, each // 8))
            pack[first_pack[j] + p] = made[-1]
        span = pl.ds(first_pack[j], packs)
        send(pack.at[span], left_in.at[span], left_s.at[j], left_r.at[j], (face, t_rt, lev))
        send(pack.at[span], right_in.at[span], right_s.at[j], right_r.at[j], (face, t_lf, lev))
        return made

    source = [unit - 2, unit - 1, 0, 1]

    def ship_corners(which, made):
        for d in range(4):
            out = jnp.zeros((8, columns), f32)
            for p, value in enumerate(made):
                out = jnp.where(within == p, pltpu.roll(value, (p - source[d]) % columns, 1), out)
            corner[which, d] = out
            send(corner.at[which, d], corner_in.at[which, d], corner_s.at[which, d],
                 corner_r.at[which, d], diagonals[d])

    east = [level_rows(wind.at[0], a) for a in range(rows)]
    north = [level_rows(wind.at[1], a) for a in range(rows)]
    speed = None
    whole = max(c[1] for c in chunks)
    for a in range(rows):
        aa = jac[a] * (m[0][a] * east[a] + m[1][a] * north[a])
        bb = jac[a] * (m[2][a] * east[a] + m[3][a] * north[a])
        aw, bw = (aa * w_col)[:levels], (bb * wr[a])[:levels]
        for k in range(-(-whole // levels)):
            n = min(levels, whole - k * levels)
            a_ref[a, k * levels : k * levels + n, :] = aw[:n]
            b_ref[a, k * levels : k * levels + n, :] = bw[:n]
        spacing = jnp.sqrt(
            m[0][a] * m[0][a] + m[1][a] * m[1][a] + m[2][a] * m[2][a] + m[3][a] * m[3][a]
        )
        here = jnp.max(east[a] * east[a] + north[a] * north[a], axis=0, keepdims=True)
        here = jnp.sqrt(here) * spacing
        speed = here if speed is None else jnp.maximum(speed, here)

    depth = [level_rows(thick, a) for a in range(rows)]
    depth_c = by_column(depth)
    flux_a, flux_b = [], []
    for a in range(rows):
        dr, dc = along_rows(depth, a, dd[a % 4]), depth_c[a]
        gx, gy = m[0][a] * dr + m[2][a] * dc, m[1][a] * dr + m[3][a] * dc
        flux_a.append(jac[a] * (m[0][a] * gx + m[1][a] * gy))
        flux_b.append(jac[a] * (m[2][a] * gx + m[3][a] * gy))
    flux_c = by_column(flux_b)
    damp = None
    for a in range(rows):
        lap = jnp.abs(along_rows(flux_a, a, dd[a % 4]) + flux_c[a])
        here = jnp.max(lap, axis=0, keepdims=True) / jac[a]
        damp = here if damp is None else jnp.maximum(damp, here)
    peak[0] = jnp.concatenate(
        [time_step * speed, (time_step * viscosity) * damp, jnp.zeros((6, columns), f32)], 0
    )
    peak_face = [
        send(peak.at[0], peak_in.at[o - 1], peak_s.at[o - 1], peak_r.at[o - 1],
             (lax.rem(face + o, nf), tile, lev))
        for o in range(1, nf)
    ]
    warm = [level_rows(temp, a) for a in range(rows)]
    warm_c = by_column(warm)
    value = []
    for a in range(rows):
        dr, dc = along_rows(warm, a, dd[a % 4]), warm_c[a]
        gx, gy = m[0][a] * dr + m[2][a] * dc, m[1][a] * dr + m[3][a] * dc
        value.append(mass[a] * (warm[a] - time_step * (east[a] * gx + north[a] * gy)))
    for r, x in enumerate(merged(value)):
        put(pieces[0][0], 0, r, lanes_plain(x))
    for r, x in enumerate(merged(mass)):
        put(pieces[0][0], pad, r, lanes_plain(jnp.broadcast_to(x, (8, columns))))
    first, second, keep = [], [], []
    for a in range(rows):
        aa = jac[a] * (m[0][a] * east[a] + m[1][a] * north[a])
        bb = jac[a] * (m[2][a] * east[a] + m[3][a] * north[a])
        first.append(w_col * (depth[a] * aa - viscosity * flux_a[a]))
        second.append(wr[a] * (depth[a] * bb - viscosity * flux_b[a]))
    for a in range(rows):
        keep.append(mass[a] * depth[a] - along_rows(first, a, step_d[a]))
    for r, (x, y) in enumerate(zip(merged(keep), merged(second))):
        put(pieces[0][0], pad + 8, r, lanes_both(x, y))
    made = ship(0)

    for k, (start, count, _) in enumerate(chunks):
        loads[n0 + k].wait()
        q = [tracer[pl.ds(start * rows + a, count, stride=rows), :] for a in range(rows)]
        first = [q[a] * a_ref[a, :count, :] for a in range(rows)]
        keep = [mass[a] * q[a] - along_rows(first, a, step_d[a]) for a in range(rows)]
        second = [q[a] * b_ref[a, :count, :] for a in range(rows)]
        for r, (x, y) in enumerate(zip(merged(keep), merged(second))):
            put(pieces[k + 1][0], 0, r, lanes_both(x, y))
        made += ship(k + 1)
    ship_corners(0, made)

    best = peak[0]
    for o, copy in enumerate(peak_face):
        copy.wait_recv()
        best = jnp.maximum(best, peak_in[o])
    peak[1] = best
    base = nf - 1
    peak_tile = [
        send(peak.at[1], peak_in.at[base + o - 1], peak_s.at[base + o - 1], peak_r.at[base + o - 1],
             (face, lax.rem(tile + o, nt), lev))
        for o in range(1, nt)
    ]

    above = ground[...]
    for o, copy in enumerate(totals):
        copy.wait_recv()
        origin = lax.rem(lev + nl - (o + 1), nl)
        use = jnp.where(origin > lev, 1.0, 0.0).astype(f32)
        above = above + use * total_in[o]
    energy = []
    for a in range(rows):
        u, v = level_rows(wind.at[0], a), level_rows(wind.at[1], a)
        energy.append(0.5 * (u * u + v * v) + level_rows(geo, a) + above[a : a + 1, :])
    energy_c = by_column(energy)
    value_u, value_v = [], []
    for a in range(rows):
        u, v = level_rows(wind.at[0], a), level_rows(wind.at[1], a)
        dr, dc = along_rows(energy, a, dd[a % 4]), energy_c[a]
        value_u.append(mass[a] * (u - time_step * (m[0][a] * dr + m[2][a] * dc)))
        value_v.append(mass[a] * (v - time_step * (m[1][a] * dr + m[3][a] * dc)))
    for r, (x, y) in enumerate(zip(merged(value_u), merged(value_v))):
        put(pieces[last][0], 0, r, lanes_plain(x))
        put(pieces[last][0], pad, r, lanes_plain(y))
    ship_corners(1, ship(last))

    best = peak[1]
    for o, copy in enumerate(peak_tile):
        copy.wait_recv()
        best = jnp.maximum(best, peak_in[base + o])
    peak[2] = best
    base = nf + nt - 2
    peak_lev = [
        send(peak.at[2], peak_in.at[base + o - 1], peak_s.at[base + o - 1], peak_r.at[base + o - 1],
             (face, tile, lax.rem(lev + o, nl)))
        for o in range(1, nl)
    ]

    def seam(ref, f, t, k):
        return ref[f, k, t]

    codes = [
        lax.rem(4 - seam(rot_ref, f_up, tile, 0), 4), seam(rot_ref, face, tile, 0),
        lax.rem(4 - seam(rot_ref, face, t_lf, 1), 4), seam(rot_ref, face, tile, 1),
    ]
    flips = [
        seam(flip_ref, f_up, tile, 0), seam(flip_ref, face, tile, 0),
        seam(flip_ref, face, t_lf, 1), seam(flip_ref, face, tile, 1),
    ]
    tallies = [
        tally_ref[f_up, t_lf], tally_ref[f_up, tile],
        tally_ref[face, t_lf], tally_ref[face, tile],
    ]

    def cosine(code):
        return jnp.where(code == 0, 1.0, jnp.where(code == 2, -1.0, 0.0)).astype(f32)

    def sine(code):
        return jnp.where(code == 1, 1.0, jnp.where(code == 3, -1.0, 0.0)).astype(f32)

    def filled(x):
        return jnp.full((8, columns), x)

    odd = lax.rem(lane, 2) == 1
    mirror = lane - within + (unit - 2) - 2 * (within // 2) + lax.rem(within, 2)
    mirror = jnp.clip(mirror, 0, columns - 1)
    side_flip = jnp.where(odd, filled(flips[2]), filled(flips[3])) == 1
    side_cos = jnp.where(odd, filled(cosine(codes[2])), filled(cosine(codes[3])))
    side_sin = jnp.where(odd, filled(sine(codes[2])), filled(sine(codes[3])))
    corner_code = [
        lax.rem(codes[0] + codes[2], 4), lax.rem(codes[0] + codes[3], 4),
        lax.rem(codes[1] + codes[2], 4), lax.rem(codes[1] + codes[3], 4),
    ]
    target = [1, 0, unit - 1, unit - 2]
    alive = [filled(tallies[d]) == 4 for d in range(4)]

    def sides(index):
        a, b = left_in[index], right_in[index]
        x = jnp.where(odd, pltpu.roll(a, 1, 1), pltpu.roll(b, columns - 1, 1))
        return jnp.where(side_flip, jnp.take_along_axis(x, mirror, axis=1), x)

    def corner_values(which, d, p):
        x = pltpu.roll(corner_in[which, d], (target[d] - p) % columns, 1)
        return jnp.where(alive[d] & (within == target[d]), x, 0.0)

    edge = (lane[:1] == 0) | (lane[:1] == columns - 1)

    def to_edges(x, i, r):
        y = pltpu.roll(x, (columns - (unit * i + 2 * r + 1)) % columns, 1)
        return jnp.where(edge, y, 0.0)

    rev = (columns - 1) - lax.broadcasted_iota(jnp.int32, (8, columns), 1)
    row_flip = [filled(flips[0]) == 1, filled(flips[1]) == 1]

    def row_rim(ref, which, start, groups):
        out = []
        for i in range(groups):
            x = ref[start + 8 * i : start + 8 * i + 8, :]
            out.append(jnp.where(row_flip[which], jnp.take_along_axis(x, rev, axis=1), x))
        return out

    def arrived(j, corners):
        start, count, packs = pieces[j]
        span, pspan = pl.ds(start, count), pl.ds(first_pack[j], packs)

        def wait(src, dst, s, r, to):
            pltpu.make_async_remote_copy(
                src_ref=src, dst_ref=dst, send_sem=s, recv_sem=r, device_id=to, device_id_type=MESH
            ).wait_recv()

        wait(z_ref.at[distinct - 1, span], up_in.at[span], up_s.at[j], up_r.at[j], (f_dn, tile, lev))
        wait(z_ref.at[0, span], down_in.at[span], down_s.at[j], down_r.at[j], (f_up, tile, lev))
        wait(pack.at[pspan], left_in.at[pspan], left_s.at[j], left_r.at[j], (face, t_rt, lev))
        wait(pack.at[pspan], right_in.at[pspan], right_s.at[j], right_r.at[j], (face, t_lf, lev))
        if corners is not None:
            for d in range(4):
                wait(corner.at[corners, d], corner_in.at[corners, d], corner_s.at[corners, d],
                     corner_r.at[corners, d], diagonals[d])

    def finished(start, i, r, side, i_side, top, bottom):
        x = z_ref[r, start + 8 * i : start + 8 * i + 8, :] + to_edges(side, i_side, r)
        if r == 0:
            x = x + top
        if r == distinct - 1:
            x = x + bottom
        return x

    def store(ref, begin, i, valid, r, x):
        n = min(8, valid - 8 * i)
        if n <= 0:
            return
        for a in range(rows):
            if rep[a] == r:
                ref[pl.ds((begin + 8 * i) * rows + a, n, stride=rows), :] = (x * inverse[a])[:n]

    arrived(0, 0)
    x = sides(first_pack[0])
    for d in range(4):
        x = x + corner_values(0, d, 0)
    groups = pad // 8
    top, bottom = row_rim(up_in, 0, 0, 2 * groups + 1), row_rim(down_in, 1, 0, 2 * groups + 1)
    inverse = [None] * rows
    for r in range(distinct):
        whole_mass = 1.0 / finished(0, groups, r, x, groups, top[groups], bottom[groups])
        for a in range(rows):
            if rep[a] == r:
                inverse[a] = whole_mass
    for i in range(groups):
        for r in range(distinct):
            store(temp_o, 0, i, levels, r, finished(0, i, r, x, i, top[i], bottom[i]))
            j = groups + 1 + i
            store(thick_o, 0, i, levels, r, finished(0, j, r, x, j, top[j], bottom[j]))

    for k, (start, count, valid) in enumerate(chunks):
        j = k + 1
        arrived(j, None)
        x = sides(first_pack[j])
        for d in range(4):
            x = x + corner_values(0, d, j)
        top = row_rim(up_in, 0, pieces[j][0], count // 8)
        bottom = row_rim(down_in, 1, pieces[j][0], count // 8)
        for i in range(count // 8):
            for r in range(distinct):
                store(tracer_o, start, i, valid, r,
                      finished(pieces[j][0], i, r, x, i, top[i], bottom[i]))

    arrived(last, 1)
    p = first_pack[last]
    xu, xv = sides(p), sides(p + 1)
    xu, xv = side_cos * xu - side_sin * xv, side_sin * xu + side_cos * xv
    for d in range(4):
        cu, cv = corner_values(1, d, 0), corner_values(1, d, 1)
        c, s = cosine(corner_code[d]), sine(corner_code[d])
        xu, xv = xu + (c * cu - s * cv), xv + (s * cu + c * cv)
    begin = pieces[last][0]
    rims = []
    for which, ref in ((0, up_in), (1, down_in)):
        both = row_rim(ref, which, begin, 2 * groups)
        c, s = cosine(codes[which]), sine(codes[which])
        ru = [c * both[i] - s * both[groups + i] for i in range(groups)]
        rv = [s * both[i] + c * both[groups + i] for i in range(groups)]
        rims.append((ru, rv))
    for i in range(groups):
        for r in range(distinct):
            store(wind_o.at[0], 0, i, levels, r,
                  finished(begin, i, r, xu, i, rims[0][0][i], rims[1][0][i]))
            store(wind_o.at[1], 0, i, levels, r,
                  finished(begin + pad, i, r, xv, i, rims[0][1][i], rims[1][1][i]))

    best = peak[2]
    for o, copy in enumerate(peak_lev):
        copy.wait_recv()
        best = jnp.maximum(best, peak_in[base + o])
    bound_o[...] = best
    for copy in sent:
        copy.wait_send()


def write_out(wind, temp, thick, tracer, bound, wind_o, temp_o, thick_o, tracer_o, bound_o, sem):
    pairs = ((tracer, tracer_o), (wind, wind_o), (temp, temp_o), (thick, thick_o))
    copies = [pltpu.make_async_copy(a, b, sem.at[i]) for i, (a, b) in enumerate(pairs)]
    for copy in copies:
        copy.start()
    bound_o[0] = jnp.max(bound[0:1, :])
    bound_o[1] = jnp.max(bound[1:2, :])
    for copy in copies:
        copy.wait()


def on_device(
    sizes, wind, temp, thick, tracers, ground, maps, det, rot, flip, tally
):
    nf, nt, nl = sizes
    levels, rows, columns = temp.shape
    if rows != 8 or columns != 128:
        raise ValueError("block shape")
    count = tracers.shape[0]
    chunks = layout(levels, count)
    pad = -(-levels // 8) * 8
    table, dct, w_col = lane_tables(columns)
    distinct = rows - rows // 4 + 1
    total_rows = 4 * pad + 8 + sum(c[1] for c in chunks)
    pieces = len(chunks) + 2
    packs = len(chunks) + 3
    whole = max(c[1] for c in chunks)
    n = levels * rows
    dma = pltpu.SemaphoreType.DMA
    peers = nf + nt + nl - 3
    hbm = pl.BlockSpec(memory_space=pl.ANY)
    smem = pl.BlockSpec(memory_space=pltpu.SMEM)
    vmem = pl.BlockSpec(memory_space=pltpu.VMEM)
    last = chunks[-1]
    shapes = ((2, n, columns), (n, columns), (n, columns), (count * n, columns), (8, columns))
    outs = pl.pallas_call(
        functools.partial(kernel, sizes, (levels, rows, columns, chunks, pad)),
        out_shape=tuple(pltpu.VMEM(shape, f32) for shape in shapes),
        in_specs=[hbm] * 10 + [smem] * 3,
        out_specs=(vmem,) * 5,
        scratch_shapes=[
            pltpu.VMEM((2, pad * rows, columns), f32),
            pltpu.VMEM((pad * rows, columns), f32),
            pltpu.VMEM((pad * rows, columns), f32),
            pltpu.VMEM(((last[0] + last[1]) * rows, columns), f32),
            pltpu.VMEM((pad * rows, columns), f32),
            pltpu.VMEM((rows, columns), f32),
            pltpu.VMEM((4 * rows, columns), f32),
            pltpu.VMEM((rows, columns), f32),
            pltpu.VMEM(table.shape, bf16),
            pltpu.VMEM(dct.shape, f32),
            pltpu.VMEM((1, columns), f32),
            pltpu.VMEM((rows, whole, columns), f32),
            pltpu.VMEM((rows, whole, columns), f32),
            pltpu.VMEM((distinct, total_rows, columns), f32),
            pltpu.VMEM((packs, 8, columns), f32),
            pltpu.VMEM((2, 4, 8, columns), f32),
            pltpu.VMEM((rows, columns), f32),
            pltpu.VMEM((3, 8, columns), f32),
            pltpu.VMEM((total_rows, columns), f32),
            pltpu.VMEM((total_rows, columns), f32),
            pltpu.VMEM((packs, 8, columns), f32),
            pltpu.VMEM((packs, 8, columns), f32),
            pltpu.VMEM((2, 4, 8, columns), f32),
            pltpu.VMEM((nl - 1, rows, columns), f32),
            pltpu.VMEM((peers, 8, columns), f32),
            dma((10 + len(chunks),)),
        ]
        + [dma((pieces,))] * 8
        + [dma((2, 4))] * 2
        + [dma((nl - 1,))] * 2
        + [dma((peers,))] * 2,
        compiler_params=pltpu.CompilerParams(collective_id=0, has_side_effects=True),
    )(
        wind.reshape(2, n, columns), temp.reshape(n, columns), thick.reshape(n, columns),
        tracers.reshape(count * n, columns), ground, maps.reshape(4 * rows, columns), det,
        table, dct, w_col, rot.transpose(0, 2, 1), flip.transpose(0, 2, 1), tally,
    )
    outs = pl.pallas_call(
        write_out,
        out_shape=tuple(jax.ShapeDtypeStruct(x, f32) for x in shapes[:4] + ((2,),)),
        in_specs=[vmem] * 5,
        out_specs=(hbm,) * 4 + (smem,),
        scratch_shapes=[dma((4,))],
    )(*[pltpu.with_memory_space_constraint(x, pltpu.VMEM) for x in outs])
    return (
        outs[0].reshape(wind.shape), outs[1].reshape(temp.shape), outs[2].reshape(thick.shape),
        outs[3].reshape(tracers.shape), outs[4],
    )


def solution(mesh):
    sizes = tuple(mesh.shape[name] for name in ("face", "tile", "lev"))
    level = P("lev", "face", "tile")
    stacked = P(None, "lev", "face", "tile")
    return jax.shard_map(
        functools.partial(on_device, sizes),
        mesh=mesh,
        in_specs=(stacked, level, level, stacked, P("face", "tile"), P(None, "face", "tile"),
                  P("face", "tile"), P(), P(), P()),
        out_specs=(stacked, level, level, stacked, P()),
        check_vma=False,
    )
```

```python
import functools
import math

import jax
import jax.numpy as jnp
import numpy as np
from jax import lax
from jax.experimental import pallas as pl
from jax.experimental.pallas import tpu as pltpu
from jax.sharding import PartitionSpec as P

time_step = 0.05
viscosity = 0.05
f32 = jnp.float32
bf16 = jnp.bfloat16
MESH = pl.DeviceIdType.MESH
highest = lax.Precision.HIGHEST


def gll_tables():
    offset = 1.0 / math.sqrt(5.0)
    nodes = np.array([-1.0, -offset, offset, 1.0])
    weights = np.array([1.0 / 6.0, 5.0 / 6.0, 5.0 / 6.0, 1.0 / 6.0])
    bary = np.ones(4)
    for i in range(4):
        for j in range(4):
            if j != i:
                bary[i] = bary[i] / (nodes[i] - nodes[j])
    derivative = np.zeros((4, 4))
    for i in range(4):
        for j in range(4):
            if j != i:
                derivative[i, j] = bary[j] / bary[i] / (nodes[i] - nodes[j])
        derivative[i, i] = -np.sum(derivative[i])
    return derivative, weights


def lane_tables(columns):
    derivative, weights = gll_tables()
    d = np.kron(np.eye(columns // 4), derivative)
    s = np.eye(columns)
    for c in range(columns - 1):
        if c % 4 == 3:
            s[c, c + 1] = s[c + 1, c] = 1.0
    w = np.tile(weights, columns // 4)
    t = (-time_step * (d.T * w[None, :]) @ s).astype(np.float32)
    t_hi = jnp.asarray(t).astype(bf16)
    t_lo = (jnp.asarray(t) - t_hi.astype(f32)).astype(bf16)
    sb = jnp.asarray(s, bf16)
    d_t = jnp.asarray(d.T, f32)
    d_hi = d_t.astype(bf16)
    d_lo = (d_t - d_hi.astype(f32)).astype(bf16)
    return jnp.concatenate([sb, sb, t_hi, t_hi, t_lo], 0), jnp.concatenate([d_hi, d_hi, d_lo], 0), jnp.asarray(w[None, :], f32)


def split(x):
    hi = x.astype(bf16)
    return hi, (x - hi.astype(f32)).astype(bf16)


def layout(levels, tracers):
    group = 8 // math.gcd(levels, 8)
    chunks, q = [], 0
    while q < tracers:
        n = min(group, tracers - q)
        chunks.append((q * levels, -(-n * levels // 8) * 8, n * levels))
        q += n
    return chunks


def kernel(
    sizes, dims,
    wind_h, temp_h, thick_h, tracer_h, ground_h, maps_h, det_h, ops_h, dct_h, wc_h,
    rot_ref, flip_ref, tally_ref,
    wind_o, temp_o, thick_o, tracer_o, bound_o,
    wind, temp, thick, tracer, geo, ground, maps, det, ops, dct, wc,
    a_ref, b_ref, z_ref, pack, corner, total, peak,
    up_in, down_in, left_in, right_in, corner_in, total_in, peak_in,
    in_sem, up_s, up_r, down_s, down_r, left_s, left_r, right_s, right_r,
    corner_s, corner_r, total_s, total_r, peak_s, peak_r,
):
    nf, nt, nl = sizes
    levels, rows, columns, chunks, pad = dims
    derivative, weights = gll_tables()
    rep = [a - (a // 4) for a in range(rows)]
    distinct = rows - rows // 4 + 1
    face, tile, lev = lax.axis_index("face"), lax.axis_index("tile"), lax.axis_index("lev")
    f_up, f_dn = lax.rem(face + nf - 1, nf), lax.rem(face + 1, nf)
    t_lf, t_rt = lax.rem(tile + nt - 1, nt), lax.rem(tile + 1, nt)

    pieces = [(0, 8, 1)]
    at = 8
    for _, count, _ in chunks:
        pieces.append((at, count, 1))
        at += count
    pieces.append((at, 2 * pad, 1))
    pieces.append((at + 2 * pad, 2 * pad, 2))
    first_pack = np.cumsum([0] + [p[2] for p in pieces]).tolist()
    last = len(pieces) - 1
    heat = last - 1

    local = [
        (temp_h, temp.at[: levels * rows]), (thick_h, thick.at[: levels * rows]),
        (wind_h.at[0], wind.at[0, : levels * rows]), (wind_h.at[1], wind.at[1, : levels * rows]),
        (maps_h, maps), (det_h, det), (wc_h, wc), (ground_h, ground), (dct_h, dct), (ops_h, ops),
    ]
    loads = [pltpu.make_async_copy(s, d, in_sem.at[i]) for i, (s, d) in enumerate(local)]
    n0 = len(local)
    for k, (start, _, valid) in enumerate(chunks):
        span = pl.ds(start * rows, valid * rows)
        loads.append(pltpu.make_async_copy(tracer_h.at[span], tracer.at[span], in_sem.at[n0 + k]))
    for load in loads:
        load.start()

    peers = [(lax.rem(face + o, nf), tile, lev) for o in range(1, nf)]
    peers += [(face, lax.rem(tile + o, nt), lev) for o in range(1, nt)]
    peers += [(face, tile, lax.rem(lev + o, nl)) for o in range(1, nl)]
    diagonals = [(f_dn, t_rt, lev), (f_dn, t_lf, lev), (f_up, t_rt, lev), (f_up, t_lf, lev)]
    barrier = pltpu.get_barrier_semaphore()
    for peer in peers + diagonals:
        pl.semaphore_signal(barrier, inc=1, device_id=peer, device_id_type=MESH)

    extra = (pad - levels) * rows
    if extra:
        zero = jnp.zeros((extra, columns), f32)
        temp[levels * rows :, :] = zero
        thick[levels * rows :, :] = zero
        geo[levels * rows :, :] = zero
        wind[0, levels * rows :, :] = zero
        wind[1, levels * rows :, :] = zero
    end = chunks[-1][0] + chunks[-1][2]
    more = chunks[-1][1] - chunks[-1][2]
    if more:
        tracer[end * rows :, :] = jnp.zeros((more * rows, columns), f32)

    sent = []

    def send(src, dst, s, r, to):
        copy = pltpu.make_async_remote_copy(
            src_ref=src, dst_ref=dst, send_sem=s, recv_sem=r, device_id=to, device_id_type=MESH
        )
        copy.start()
        sent.append(copy)
        return copy

    loads[0].wait()
    loads[1].wait()
    acc = jnp.zeros((rows, columns), f32)
    for k in reversed(range(levels)):
        term = temp[k * rows : (k + 1) * rows, :] * thick[k * rows : (k + 1) * rows, :]
        geo[k * rows : (k + 1) * rows, :] = acc + 0.5 * term
        acc = acc + term
    total[...] = acc
    pl.semaphore_wait(barrier, len(peers) + len(diagonals))
    totals = [
        send(total, total_in.at[o - 1], total_s.at[o - 1], total_r.at[o - 1],
             (face, tile, lax.rem(lev + o, nl)))
        for o in range(1, nl)
    ]
    for load in loads[2:n0]:
        load.wait()
    w_col = wc[...]
    table = ops[...]
    narrow = ops[: 2 * columns, :]
    wr = [float(weights[a % 4]) for a in range(rows)]
    m = [[maps[e * rows + a : e * rows + a + 1, :] for a in range(rows)] for e in range(4)]
    jac = [det[a : a + 1, :] for a in range(rows)]
    mass = [jac[a] * (wr[a] * w_col) for a in range(rows)]
    step_d = [[float(time_step * wr[a] * derivative[a % 4, b]) for b in range(4)] for a in range(rows)]
    dd = [[float(derivative[i, j]) for j in range(4)] for i in range(4)]

    def level_rows(ref, a):
        return ref[pl.ds(a, pad, stride=rows), :]

    def along_rows(values, a, coef):
        base = a - a % 4
        out = coef[0] * values[base]
        for b in range(1, 4):
            out = out + coef[b] * values[base + b]
        return out

    def merged(values):
        out = [None] * distinct
        for a in range(rows):
            r = rep[a]
            out[r] = values[a] if out[r] is None else out[r] + values[a]
        return out

    def lanes_plain(x):
        hi, lo = split(x)
        return jnp.dot(jnp.concatenate([hi, lo], 1), narrow, preferred_element_type=f32)

    def lanes_both(p, g):
        ph, plo = split(p)
        gh, glo = split(g)
        return jnp.dot(
            jnp.concatenate([ph, plo, gh, glo, gh], 1), table, preferred_element_type=f32
        )

    def by_column(values):
        stacked = jnp.concatenate(values, 0)
        hi, lo = split(stacked)
        out = jnp.dot(
            jnp.concatenate([hi, lo, hi], 1), dct[...], preferred_element_type=f32
        )
        n = values[0].shape[0]
        return [out[i * n : (i + 1) * n] for i in range(len(values))]

    lane = lax.broadcasted_iota(jnp.int32, (8, columns), 1)
    unit = 2 * distinct
    within = lax.rem(lane, unit)

    def put(piece, offset, r, z):
        z_ref[r, piece + offset : piece + offset + z.shape[0], :] = z

    def pack_of(start, groups):
        out = jnp.zeros((8, columns), f32)
        for i in range(groups):
            for r in range(distinct):
                spot = unit * i + 2 * r
                value = pltpu.roll(z_ref[r, start + 8 * i : start + 8 * i + 8, :], spot + 1, 1)
                out = jnp.where((lane == spot) | (lane == spot + 1), value, out)
        return out

    def ship_rows(j):
        start, count, _ = pieces[j]
        span = pl.ds(start, count)
        send(z_ref.at[distinct - 1, span], up_in.at[span], up_s.at[j], up_r.at[j], (f_dn, tile, lev))
        send(z_ref.at[0, span], down_in.at[span], down_s.at[j], down_r.at[j], (f_up, tile, lev))

    def ship_sides(j):
        start, count, packs = pieces[j]
        each = count // packs
        made = []
        for p in range(packs):
            made.append(pack_of(start + p * each, each // 8))
            pack[first_pack[j] + p] = made[-1]
        span = pl.ds(first_pack[j], packs)
        send(pack.at[span], left_in.at[span], left_s.at[j], left_r.at[j], (face, t_rt, lev))
        send(pack.at[span], right_in.at[span], right_s.at[j], right_r.at[j], (face, t_lf, lev))
        return made

    source = [unit - 2, unit - 1, 0, 1]

    def ship_corners(which, made):
        for d in range(4):
            out = jnp.zeros((8, columns), f32)
            for p, value in enumerate(made):
                out = jnp.where(within == p, pltpu.roll(value, (p - source[d]) % columns, 1), out)
            corner[which, d] = out
            send(corner.at[which, d], corner_in.at[which, d], corner_s.at[which, d],
                 corner_r.at[which, d], diagonals[d])

    east = [level_rows(wind.at[0], a) for a in range(rows)]
    north = [level_rows(wind.at[1], a) for a in range(rows)]
    speed, parts = None, []
    whole = max(c[1] for c in chunks)
    for a in range(rows):
        aa = jac[a] * (m[0][a] * east[a] + m[1][a] * north[a])
        bb = jac[a] * (m[2][a] * east[a] + m[3][a] * north[a])
        parts.append(((aa * w_col)[:levels], (bb * wr[a])[:levels]))
        spacing = jnp.sqrt(
            m[0][a] * m[0][a] + m[1][a] * m[1][a] + m[2][a] * m[2][a] + m[3][a] * m[3][a]
        )
        here = jnp.max(east[a] * east[a] + north[a] * north[a], axis=0, keepdims=True)
        here = jnp.sqrt(here) * spacing
        speed = here if speed is None else jnp.maximum(speed, here)

    @pl.when(face < nf)
    def _():
        for a, pair in enumerate(parts):
            for k in range(-(-whole // levels)):
                n = min(levels, whole - k * levels)
                a_ref[a, k * levels : k * levels + n, :] = pair[0][:n]
                b_ref[a, k * levels : k * levels + n, :] = pair[1][:n]

    def tracers_of(k):
        start, count, _ = chunks[k]
        loads[n0 + k].wait()
        q = [tracer[pl.ds(start * rows + a, count, stride=rows), :] for a in range(rows)]
        first = [q[a] * a_ref[a, :count, :] for a in range(rows)]
        keep = [mass[a] * q[a] - along_rows(first, a, step_d[a]) for a in range(rows)]
        second = [q[a] * b_ref[a, :count, :] for a in range(rows)]
        for r, (x, y) in enumerate(zip(merged(keep), merged(second))):
            put(pieces[k + 1][0], 0, r, lanes_both(x, y))

    depth = [level_rows(thick, a) for a in range(rows)]
    depth_c = by_column(depth)
    flux_a, flux_b = [], []
    for a in range(rows):
        dr, dc = along_rows(depth, a, dd[a % 4]), depth_c[a]
        gx, gy = m[0][a] * dr + m[2][a] * dc, m[1][a] * dr + m[3][a] * dc
        flux_a.append(jac[a] * (m[0][a] * gx + m[1][a] * gy))
        flux_b.append(jac[a] * (m[2][a] * gx + m[3][a] * gy))
    flux_c = by_column(flux_b)
    damp = None
    for a in range(rows):
        lap = jnp.abs(along_rows(flux_a, a, dd[a % 4]) + flux_c[a])
        here = jnp.max(lap, axis=0, keepdims=True) / jac[a]
        damp = here if damp is None else jnp.maximum(damp, here)
    peak[0] = jnp.concatenate(
        [time_step * speed, (time_step * viscosity) * damp, jnp.zeros((6, columns), f32)], 0
    )
    peak_face = [
        send(peak.at[0], peak_in.at[o - 1], peak_s.at[o - 1], peak_r.at[o - 1],
             (lax.rem(face + o, nf), tile, lev))
        for o in range(1, nf)
    ]

    early = min(3, len(chunks))
    for r, x in enumerate(merged(mass)):
        put(0, 0, r, lanes_plain(jnp.broadcast_to(x, (8, columns))))
    ship_rows(0)
    ship_corners(0, ship_sides(0))
    tracers_of(0)
    ship_rows(1)
    made = ship_sides(1)
    for k in range(1, early):
        tracers_of(k)
        ship_rows(k + 1)
        made += ship_sides(k + 1)

    first, second, keep = [], [], []
    for a in range(rows):
        aa = jac[a] * (m[0][a] * east[a] + m[1][a] * north[a])
        bb = jac[a] * (m[2][a] * east[a] + m[3][a] * north[a])
        first.append(w_col * (depth[a] * aa - viscosity * flux_a[a]))
        second.append(wr[a] * (depth[a] * bb - viscosity * flux_b[a]))
    for a in range(rows):
        keep.append(mass[a] * depth[a] - along_rows(first, a, step_d[a]))
    for r, (x, y) in enumerate(zip(merged(keep), merged(second))):
        put(pieces[heat][0], pad, r, lanes_both(x, y))
    warm = [level_rows(temp, a) for a in range(rows)]
    warm_c = by_column(warm)
    value = []
    for a in range(rows):
        dr, dc = along_rows(warm, a, dd[a % 4]), warm_c[a]
        gx, gy = m[0][a] * dr + m[2][a] * dc, m[1][a] * dr + m[3][a] * dc
        value.append(mass[a] * (warm[a] - time_step * (east[a] * gx + north[a] * gy)))
    for r, x in enumerate(merged(value)):
        put(pieces[heat][0], 0, r, lanes_plain(x))
    dynamic = ship_sides(heat)

    for k in range(early, len(chunks)):
        tracers_of(k)
        made += ship_sides(k + 1)
    ship_corners(1, made)

    above = ground[...]
    for o, copy in enumerate(totals):
        copy.wait_recv()
        origin = lax.rem(lev + nl - (o + 1), nl)
        use = jnp.where(origin > lev, 1.0, 0.0).astype(f32)
        above = above + use * total_in[o]
    energy = []
    for a in range(rows):
        u, v = level_rows(wind.at[0], a), level_rows(wind.at[1], a)
        energy.append(0.5 * (u * u + v * v) + level_rows(geo, a) + above[a : a + 1, :])
    energy_c = by_column(energy)
    value_u, value_v = [], []
    for a in range(rows):
        u, v = level_rows(wind.at[0], a), level_rows(wind.at[1], a)
        dr, dc = along_rows(energy, a, dd[a % 4]), energy_c[a]
        value_u.append(mass[a] * (u - time_step * (m[0][a] * dr + m[2][a] * dc)))
        value_v.append(mass[a] * (v - time_step * (m[1][a] * dr + m[3][a] * dc)))
    for r, (x, y) in enumerate(zip(merged(value_u), merged(value_v))):
        put(pieces[last][0], 0, r, lanes_plain(x))
        put(pieces[last][0], pad, r, lanes_plain(y))
    dynamic += ship_sides(last)
    ship_corners(2, dynamic)
    ship_rows(last)
    for k in range(early, len(chunks)):
        ship_rows(k + 1)
    ship_rows(heat)

    def second_stage():
        best = peak[0]
        for o, copy in enumerate(peak_face):
            copy.wait_recv()
            best = jnp.maximum(best, peak_in[o])
        peak[1] = best
        base = nf - 1
        return [
            send(peak.at[1], peak_in.at[base + o - 1], peak_s.at[base + o - 1],
                 peak_r.at[base + o - 1], (face, lax.rem(tile + o, nt), lev))
            for o in range(1, nt)
        ]

    def third_stage(peak_tile):
        best = peak[1]
        base = nf - 1
        for o, copy in enumerate(peak_tile):
            copy.wait_recv()
            best = jnp.maximum(best, peak_in[base + o])
        peak[2] = best
        base = nf + nt - 2
        return [
            send(peak.at[2], peak_in.at[base + o - 1], peak_s.at[base + o - 1],
                 peak_r.at[base + o - 1], (face, tile, lax.rem(lev + o, nl)))
            for o in range(1, nl)
        ]

    def seam(ref, f, t, k):
        return ref[f, k, t]

    codes = [
        lax.rem(4 - seam(rot_ref, f_up, tile, 0), 4), seam(rot_ref, face, tile, 0),
        lax.rem(4 - seam(rot_ref, face, t_lf, 1), 4), seam(rot_ref, face, tile, 1),
    ]
    flips = [
        seam(flip_ref, f_up, tile, 0), seam(flip_ref, face, tile, 0),
        seam(flip_ref, face, t_lf, 1), seam(flip_ref, face, tile, 1),
    ]
    tallies = [
        tally_ref[f_up, t_lf], tally_ref[f_up, tile],
        tally_ref[face, t_lf], tally_ref[face, tile],
    ]

    def cosine(code):
        return jnp.where(code == 0, 1.0, jnp.where(code == 2, -1.0, 0.0)).astype(f32)

    def sine(code):
        return jnp.where(code == 1, 1.0, jnp.where(code == 3, -1.0, 0.0)).astype(f32)

    def filled(x):
        return jnp.full((8, columns), x)

    odd = lax.rem(lane, 2) == 1
    mirror = lane - within + (unit - 2) - 2 * (within // 2) + lax.rem(within, 2)
    mirror = jnp.clip(mirror, 0, columns - 1)
    side_flip = jnp.where(odd, filled(flips[2]), filled(flips[3])) == 1
    side_cos = jnp.where(odd, filled(cosine(codes[2])), filled(cosine(codes[3])))
    side_sin = jnp.where(odd, filled(sine(codes[2])), filled(sine(codes[3])))
    corner_code = [
        lax.rem(codes[0] + codes[2], 4), lax.rem(codes[0] + codes[3], 4),
        lax.rem(codes[1] + codes[2], 4), lax.rem(codes[1] + codes[3], 4),
    ]
    target = [1, 0, unit - 1, unit - 2]
    alive = [filled(tallies[d]) == 4 for d in range(4)]

    def sides(index):
        a, b = left_in[index], right_in[index]
        x = jnp.where(odd, pltpu.roll(a, 1, 1), pltpu.roll(b, columns - 1, 1))
        return jnp.where(side_flip, jnp.take_along_axis(x, mirror, axis=1), x)

    def corner_values(which, d, p):
        x = pltpu.roll(corner_in[which, d], (target[d] - p) % columns, 1)
        return jnp.where(alive[d] & (within == target[d]), x, 0.0)

    groups = pad // 8
    edge = (lane[:1] == 0) | (lane[:1] == columns - 1)

    def to_edges(x, i, r):
        y = pltpu.roll(x, (columns - (unit * i + 2 * r + 1)) % columns, 1)
        return jnp.where(edge, y, 0.0)

    rev = (columns - 1) - lax.broadcasted_iota(jnp.int32, (8, columns), 1)
    row_flip = [filled(flips[0]) == 1, filled(flips[1]) == 1]

    def row_rim(ref, which, start, groups):
        out = []
        for i in range(groups):
            x = ref[start + 8 * i : start + 8 * i + 8, :]
            out.append(jnp.where(row_flip[which], jnp.take_along_axis(x, rev, axis=1), x))
        return out

    def arrived(j, corners=None):
        start, count, packs = pieces[j]
        span, pspan = pl.ds(start, count), pl.ds(first_pack[j], packs)

        def wait(src, dst, s, r, to):
            pltpu.make_async_remote_copy(
                src_ref=src, dst_ref=dst, send_sem=s, recv_sem=r, device_id=to, device_id_type=MESH
            ).wait_recv()

        wait(z_ref.at[distinct - 1, span], up_in.at[span], up_s.at[j], up_r.at[j], (f_dn, tile, lev))
        wait(z_ref.at[0, span], down_in.at[span], down_s.at[j], down_r.at[j], (f_up, tile, lev))
        wait(pack.at[pspan], left_in.at[pspan], left_s.at[j], left_r.at[j], (face, t_rt, lev))
        wait(pack.at[pspan], right_in.at[pspan], right_s.at[j], right_r.at[j], (face, t_lf, lev))
        if corners is not None:
            for d in range(4):
                wait(corner.at[corners, d], corner_in.at[corners, d], corner_s.at[corners, d],
                     corner_r.at[corners, d], diagonals[d])

    def finished(start, i, r, side, i_side, top, bottom):
        x = z_ref[r, start + 8 * i : start + 8 * i + 8, :] + to_edges(side, i_side, r)
        if r == 0:
            x = x + top
        if r == distinct - 1:
            x = x + bottom
        return x

    def store(ref, begin, i, valid, r, x):
        n = min(8, valid - 8 * i)
        if n <= 0:
            return
        for a in range(rows):
            if rep[a] == r:
                ref[pl.ds((begin + 8 * i) * rows + a, n, stride=rows), :] = (x * inverse[a])[:n]

    arrived(0, 0)
    x = sides(0)
    for d in range(4):
        x = x + corner_values(0, d, 0)
    top, bottom = row_rim(up_in, 0, 0, 1), row_rim(down_in, 1, 0, 1)
    inverse = [None] * rows
    for r in range(distinct):
        whole_mass = 1.0 / finished(0, 0, r, x, 0, top[0], bottom[0])
        for a in range(rows):
            if rep[a] == r:
                inverse[a] = whole_mass

    def finish_tracers(k):
        start, count, valid = chunks[k]
        j = k + 1
        arrived(j, 1 if k == 0 else None)
        x = sides(first_pack[j])
        for d in range(4):
            x = x + corner_values(1, d, k)
        top = row_rim(up_in, 0, pieces[j][0], count // 8)
        bottom = row_rim(down_in, 1, pieces[j][0], count // 8)
        for i in range(count // 8):
            for r in range(distinct):
                store(tracer_o, start, i, valid, r,
                      finished(pieces[j][0], i, r, x, i, top[i], bottom[i]))

    peak_tile = second_stage()
    finish_tracers(0)
    for k in range(1, early):
        finish_tracers(k)
    peak_lev = third_stage(peak_tile)

    arrived(last, 2)
    p = first_pack[last]
    xu, xv = sides(p), sides(p + 1)
    xu, xv = side_cos * xu - side_sin * xv, side_sin * xu + side_cos * xv
    for d in range(4):
        cu, cv = corner_values(2, d, 1), corner_values(2, d, 2)
        c, s = cosine(corner_code[d]), sine(corner_code[d])
        xu, xv = xu + (c * cu - s * cv), xv + (s * cu + c * cv)
    begin = pieces[last][0]
    rims = []
    for which, ref in ((0, up_in), (1, down_in)):
        both = row_rim(ref, which, begin, 2 * groups)
        c, s = cosine(codes[which]), sine(codes[which])
        ru = [c * both[i] - s * both[groups + i] for i in range(groups)]
        rv = [s * both[i] + c * both[groups + i] for i in range(groups)]
        rims.append((ru, rv))
    for i in range(groups):
        for r in range(distinct):
            store(wind_o.at[0], 0, i, levels, r,
                  finished(begin, i, r, xu, i, rims[0][0][i], rims[1][0][i]))
            store(wind_o.at[1], 0, i, levels, r,
                  finished(begin + pad, i, r, xv, i, rims[0][1][i], rims[1][1][i]))

    for k in range(early, len(chunks)):
        finish_tracers(k)

    arrived(heat)
    begin = pieces[heat][0]
    x = sides(first_pack[heat])
    for d in range(4):
        x = x + corner_values(2, d, 0)
    top, bottom = row_rim(up_in, 0, begin, 2 * groups), row_rim(down_in, 1, begin, 2 * groups)
    for i in range(groups):
        for r in range(distinct):
            store(temp_o, 0, i, levels, r, finished(begin, i, r, x, i, top[i], bottom[i]))
            j = groups + i
            store(thick_o, 0, i, levels, r, finished(begin, j, r, x, j, top[j], bottom[j]))

    base = nf + nt - 2
    best = peak[2]
    for o, copy in enumerate(peak_lev):
        copy.wait_recv()
        best = jnp.maximum(best, peak_in[base + o])
    bound_o[...] = best
    for copy in sent:
        copy.wait_send()


def write_out(wind, temp, thick, tracer, bound, wind_o, temp_o, thick_o, tracer_o, bound_o, sem):
    pairs = ((tracer, tracer_o), (wind, wind_o), (temp, temp_o), (thick, thick_o))
    copies = [pltpu.make_async_copy(a, b, sem.at[i]) for i, (a, b) in enumerate(pairs)]
    for copy in copies:
        copy.start()
    bound_o[0] = jnp.max(bound[0:1, :])
    bound_o[1] = jnp.max(bound[1:2, :])
    for copy in copies:
        copy.wait()


def on_device(
    sizes, wind, temp, thick, tracers, ground, maps, det, rot, flip, tally
):
    nf, nt, nl = sizes
    levels, rows, columns = temp.shape
    if rows != 8 or columns != 128:
        raise ValueError("block shape")
    count = tracers.shape[0]
    chunks = layout(levels, count)
    pad = -(-levels // 8) * 8
    table, dct, w_col = lane_tables(columns)
    distinct = rows - rows // 4 + 1
    total_rows = 4 * pad + 8 + sum(c[1] for c in chunks)
    pieces = len(chunks) + 3
    packs = len(chunks) + 4
    whole = max(c[1] for c in chunks)
    n = levels * rows
    dma = pltpu.SemaphoreType.DMA
    peers = nf + nt + nl - 3
    hbm = pl.BlockSpec(memory_space=pl.ANY)
    smem = pl.BlockSpec(memory_space=pltpu.SMEM)
    vmem = pl.BlockSpec(memory_space=pltpu.VMEM)
    last = chunks[-1]
    shapes = ((2, n, columns), (n, columns), (n, columns), (count * n, columns), (8, columns))
    outs = pl.pallas_call(
        functools.partial(kernel, sizes, (levels, rows, columns, chunks, pad)),
        out_shape=tuple(pltpu.VMEM(shape, f32) for shape in shapes),
        in_specs=[hbm] * 10 + [smem] * 3,
        out_specs=(vmem,) * 5,
        scratch_shapes=[
            pltpu.VMEM((2, pad * rows, columns), f32),
            pltpu.VMEM((pad * rows, columns), f32),
            pltpu.VMEM((pad * rows, columns), f32),
            pltpu.VMEM(((last[0] + last[1]) * rows, columns), f32),
            pltpu.VMEM((pad * rows, columns), f32),
            pltpu.VMEM((rows, columns), f32),
            pltpu.VMEM((4 * rows, columns), f32),
            pltpu.VMEM((rows, columns), f32),
            pltpu.VMEM(table.shape, bf16),
            pltpu.VMEM(dct.shape, bf16),
            pltpu.VMEM((1, columns), f32),
            pltpu.VMEM((rows, whole, columns), f32),
            pltpu.VMEM((rows, whole, columns), f32),
            pltpu.VMEM((distinct, total_rows, columns), f32),
            pltpu.VMEM((packs, 8, columns), f32),
            pltpu.VMEM((3, 4, 8, columns), f32),
            pltpu.VMEM((rows, columns), f32),
            pltpu.VMEM((3, 8, columns), f32),
            pltpu.VMEM((total_rows, columns), f32),
            pltpu.VMEM((total_rows, columns), f32),
            pltpu.VMEM((packs, 8, columns), f32),
            pltpu.VMEM((packs, 8, columns), f32),
            pltpu.VMEM((3, 4, 8, columns), f32),
            pltpu.VMEM((nl - 1, rows, columns), f32),
            pltpu.VMEM((peers, 8, columns), f32),
            dma((10 + len(chunks),)),
        ]
        + [dma((pieces,))] * 8
        + [dma((3, 4))] * 2
        + [dma((nl - 1,))] * 2
        + [dma((peers,))] * 2,
        compiler_params=pltpu.CompilerParams(collective_id=0, has_side_effects=True),
    )(
        wind.reshape(2, n, columns), temp.reshape(n, columns), thick.reshape(n, columns),
        tracers.reshape(count * n, columns), ground, maps.reshape(4 * rows, columns), det,
        table, dct, w_col, rot.transpose(0, 2, 1), flip.transpose(0, 2, 1), tally,
    )
    outs = pl.pallas_call(
        write_out,
        out_shape=tuple(jax.ShapeDtypeStruct(x, f32) for x in shapes[:4] + ((2,),)),
        in_specs=[vmem] * 5,
        out_specs=(hbm,) * 4 + (smem,),
        scratch_shapes=[dma((4,))],
    )(*[pltpu.with_memory_space_constraint(x, pltpu.VMEM) for x in outs])
    return (
        outs[0].reshape(wind.shape), outs[1].reshape(temp.shape), outs[2].reshape(thick.shape),
        outs[3].reshape(tracers.shape), outs[4],
    )


def solution(mesh):
    sizes = tuple(mesh.shape[name] for name in ("face", "tile", "lev"))
    level = P("lev", "face", "tile")
    stacked = P(None, "lev", "face", "tile")
    return jax.shard_map(
        functools.partial(on_device, sizes),
        mesh=mesh,
        in_specs=(stacked, level, level, stacked, P("face", "tile"), P(None, "face", "tile"),
                  P("face", "tile"), P(), P(), P()),
        out_specs=(stacked, level, level, stacked, P()),
        check_vma=False,
    )
```
